8 devices in a mesh: dp: 2 (over z, y), tp: 4 (over x, core).
Axes of the slice: x: 2, y: 2, z: 1, core: 2. Of those that a mesh axis runs over, the one named last changes fastest.
Arguments:
- hidden: bfloat16 [512, 3072], P('dp'), parts along dimension 0
- positions: int32 [512], P('dp'), parts along dimension 0
- k_cache: bfloat16 [2, 512, 128, 8, 128], P(None, 'dp', None, 'tp'), parts along dimension 1
- v_cache: bfloat16 [2, 512, 128, 8, 128], P(None, 'dp', None, 'tp'), parts along dimension 1
- attn_norm: bfloat16 [2, 3072], replicated
- w_query: bfloat16 [2, 3072, 3072], P(None, None, 'tp')
- w_key: bfloat16 [2, 3072, 1024], P(None, None, 'tp')
- w_value: bfloat16 [2, 3072, 1024], P(None, None, 'tp')
- w_out: bfloat16 [2, 3072, 3072], P(None, 'tp')
- mlp_norm: bfloat16 [2, 3072], replicated
- w_gate: bfloat16 [2, 3072, 8192], P(None, None, 'tp')
- w_up: bfloat16 [2, 3072, 8192], P(None, None, 'tp')
- w_down: bfloat16 [2, 8192, 3072], P(None, 'tp')
Outputs:
- output 1: bfloat16 [512, 3072], P('dp'), parts along dimension 0
- output 2: bfloat16 [2, 512, 128, 8, 128], P(None, 'dp', None, 'tp'), parts along dimension 1
- output 3: bfloat16 [2, 512, 128, 8, 128], P(None, 'dp', None, 'tp'), parts along dimension 1
There are 2 independent parts. The reference program is written for one: setup_inputs(seed, part) draws one part's arguments, and reference() takes and returns one part's arrays. A program takes and returns all parts, laid end to end along the dimension named above; an argument that names none is the same for every part.
All inputs are finite; a program needn't handle non-finite values.
Results may differ from the reference program's by a relative error of at most 0.02.
Values are sent between devices in bfloat16 or wider.
A program may use at most 1 GiB of HBM per device.

```python
import math
import jax
import jax.numpy as jnp
from jax import lax

LAYERS = 2
BATCH = 256
SEQ = 128
D = 3072
HEADS = 24
KV_HEADS = 8
HEAD = 128
FF = 8192


def normal_weight(rng_key, shape, scale):
    return (jax.random.normal(rng_key, shape, jnp.float32) * scale).astype(jnp.bfloat16)


def setup_inputs(seed: int = 0, part: int = 0) -> dict:
    base_key = jax.random.key(seed)
    shared_keys = jax.random.split(base_key, 9)
    part_keys = jax.random.split(jax.random.fold_in(base_key, part), 5)
    cache_shape = (LAYERS, BATCH, SEQ, KV_HEADS, HEAD)
    drawn_pos = jax.random.randint(part_keys[1], (BATCH,), SEQ // 8, SEQ, dtype=jnp.int32)
    drawn_pos = drawn_pos.at[0].set(SEQ - 1).at[1].set(SEQ // 8)
    return dict(
        hidden=normal_weight(part_keys[0], (BATCH, D), 1.0),
        positions=jax.random.permutation(part_keys[2], drawn_pos),
        k_cache=normal_weight(part_keys[3], cache_shape, 1.0),
        v_cache=normal_weight(part_keys[4], cache_shape, 1.0),
        attn_norm=(1.0 + 0.3 * jax.random.normal(shared_keys[0], (LAYERS, D), jnp.float32)).astype(jnp.bfloat16),
        w_query=normal_weight(shared_keys[1], (LAYERS, D, HEADS * HEAD), D ** -0.5),
        w_key=normal_weight(shared_keys[2], (LAYERS, D, KV_HEADS * HEAD), 1.5 * D ** -0.5),
        w_value=normal_weight(shared_keys[3], (LAYERS, D, KV_HEADS * HEAD), 1.5 * D ** -0.5),
        w_out=normal_weight(shared_keys[4], (LAYERS, HEADS * HEAD, D), 0.5 * (SEQ / (HEADS * HEAD)) ** 0.5),
        mlp_norm=(1.0 + 0.3 * jax.random.normal(shared_keys[5], (LAYERS, D), jnp.float32)).astype(jnp.bfloat16),
        w_gate=normal_weight(shared_keys[6], (LAYERS, D, FF), D ** -0.5),
        w_up=normal_weight(shared_keys[7], (LAYERS, D, FF), D ** -0.5),
        w_down=normal_weight(shared_keys[8], (LAYERS, FF, D), 1.5 * FF ** -0.5),
    )


def rms_norm(hidden, weight):
    hidden_f32 = hidden.astype(jnp.float32)
    mean_sq = jnp.mean(hidden_f32 * hidden_f32, axis=-1, keepdims=True)
    return (hidden_f32 * lax.rsqrt(mean_sq + 1e-5) * weight.astype(jnp.float32)).astype(jnp.bfloat16)


def rope_tables(positions, head_dim):
    half_dim = head_dim // 2
    inv_freq = jnp.power(500000.0, -jnp.arange(half_dim, dtype=jnp.float32) * (2.0 / head_dim))
    wavelen = (2.0 * math.pi) / inv_freq
    smooth = (8192.0 / wavelen - 1.0) / 3.0
    blended = (1.0 - smooth) * inv_freq / 8.0 + smooth * inv_freq
    scaled = jnp.where(wavelen < 2048.0, inv_freq, jnp.where(wavelen > 8192.0, inv_freq / 8.0, blended))
    angles = positions.astype(jnp.float32)[:, None] * scaled[None, :]
    return jnp.cos(angles), jnp.sin(angles)


def apply_rope(vectors, cos_tab, sin_tab):
    half_dim = vectors.shape[-1] // 2
    vec_f32 = vectors.astype(jnp.float32)
    first = vec_f32[..., :half_dim]
    second = vec_f32[..., half_dim:]
    cos_b = cos_tab[:, None, :]
    sin_b = sin_tab[:, None, :]
    return jnp.concatenate([first * cos_b - second * sin_b, second * cos_b + first * sin_b], axis=-1).astype(jnp.bfloat16)


def attend(query, k_all, v_all, visible):
    scores = jnp.einsum('bkgd,bskd->bkgs', query.astype(jnp.float32), k_all.astype(jnp.float32)) * (query.shape[-1] ** -0.5)
    scores = jnp.where(visible, scores, -jnp.inf)
    prob_rows = jax.nn.softmax(scores, axis=-1).astype(jnp.bfloat16)
    attn_out = jnp.einsum('bkgs,bskd->bkgd', prob_rows.astype(jnp.float32), v_all.astype(jnp.float32))
    return attn_out.astype(jnp.bfloat16)


def reference(hidden, positions, k_cache, v_cache, attn_norm, w_query, w_key, w_value, w_out, mlp_norm, w_gate, w_up, w_down):
    group = HEADS // KV_HEADS
    cos_tab, sin_tab = rope_tables(positions, HEAD)
    seq_ids = jnp.arange(SEQ)
    at_pos = (seq_ids[None, :] == positions[:, None])[:, :, None, None]
    visible = (seq_ids[None, :] <= positions[:, None])[:, None, None, :]

    def layer_step(state, layer_args):
        norm_attn, wq_layer, wk_layer, wv_layer, wo_layer, norm_mlp, wg_layer, wu_layer, wd_layer, k_layer, v_layer = layer_args
        normed = rms_norm(state, norm_attn)
        query = jnp.dot(normed, wq_layer, preferred_element_type=jnp.float32).astype(jnp.bfloat16)
        key_new = jnp.dot(normed, wk_layer, preferred_element_type=jnp.float32).astype(jnp.bfloat16)
        value_new = jnp.dot(normed, wv_layer, preferred_element_type=jnp.float32).astype(jnp.bfloat16)
        query = apply_rope(query.reshape(BATCH, HEADS, HEAD), cos_tab, sin_tab)
        key_new = apply_rope(key_new.reshape(BATCH, KV_HEADS, HEAD), cos_tab, sin_tab)
        value_new = value_new.reshape(BATCH, KV_HEADS, HEAD)
        k_layer = jnp.where(at_pos, key_new[:, None], k_layer)
        v_layer = jnp.where(at_pos, value_new[:, None], v_layer)
        attended = attend(query.reshape(BATCH, KV_HEADS, group, HEAD), k_layer, v_layer, visible)
        mixed = jnp.dot(attended.reshape(BATCH, HEADS * HEAD), wo_layer, preferred_element_type=jnp.float32)
        state = state + mixed.astype(jnp.bfloat16)
        normed = rms_norm(state, norm_mlp)
        gate_proj = jnp.dot(normed, wg_layer, preferred_element_type=jnp.float32).astype(jnp.bfloat16)
        up_proj = jnp.dot(normed, wu_layer, preferred_element_type=jnp.float32).astype(jnp.bfloat16)
        activated = (jax.nn.silu(gate_proj.astype(jnp.float32)) * up_proj.astype(jnp.float32)).astype(jnp.bfloat16)
        state = state + jnp.dot(activated, wd_layer, preferred_element_type=jnp.float32).astype(jnp.bfloat16)
        return state, (k_layer, v_layer)

    stacked = (attn_norm, w_query, w_key, w_value, w_out, mlp_norm, w_gate, w_up, w_down, k_cache, v_cache)
    final, (k_out, v_out) = lax.scan(layer_step, hidden, stacked)
    return final, k_out, v_out
```

```python
import functools
import math
import jax
import jax.numpy as jnp
from jax import lax
from jax.experimental import pallas as pl
from jax.experimental.pallas import tpu as pltpu
from jax.sharding import PartitionSpec as P

BF = jnp.bfloat16
F32 = jnp.float32
MESH = pl.DeviceIdType.MESH
EPS = 1e-5
NEG = -1e30


def rope_full(positions, head_dim):
    half_dim = head_dim // 2
    inv_freq = jnp.power(500000.0, -jnp.arange(half_dim, dtype=F32) * (2.0 / head_dim))
    wavelen = (2.0 * math.pi) / inv_freq
    smooth = (8192.0 / wavelen - 1.0) / 3.0
    blended = (1.0 - smooth) * inv_freq / 8.0 + smooth * inv_freq
    scaled = jnp.where(wavelen < 2048.0, inv_freq, jnp.where(wavelen > 8192.0, inv_freq / 8.0, blended))
    angles = positions.astype(F32)[:, None] * scaled[None, :]
    cos, sin = jnp.cos(angles), jnp.sin(angles)
    return jnp.concatenate([cos, cos], axis=-1), jnp.concatenate([-sin, sin], axis=-1)


def normed(x_f32, weight_f32):
    mean_sq = jnp.mean(x_f32 * x_f32, axis=-1, keepdims=True)
    return (x_f32 * lax.rsqrt(mean_sq + EPS) * weight_f32).astype(BF)


BLK = 16
DEPTH = 8
LAG = 3


def attn_kernel(layer, aliased, pos_ref, x_ref, norm_ref, cos_ref, sin_ref, wq_hbm, wk_hbm, wv_hbm, k_hbm, v_hbm, *rest):
    if aliased:
        rest = rest[2:]
    o_ref, ko_hbm, vo_hbm, w_buf, h_buf, qkv, q_rows, k_rows, v_rows, kbuf, vbuf, wsem, insem, outsem = rest
    batch = x_ref.shape[0]
    nblk = batch // BLK
    qcols = wq_hbm.shape[2]
    kcols = wk_hbm.shape[2]
    heads = qcols // 128

    w_copies = [
        pltpu.make_async_copy(wq_hbm.at[layer], w_buf.at[:, pl.ds(0, qcols)], wsem.at[0]),
        pltpu.make_async_copy(wk_hbm.at[layer], w_buf.at[:, pl.ds(qcols, kcols)], wsem.at[1]),
        pltpu.make_async_copy(wv_hbm.at[layer], w_buf.at[:, pl.ds(qcols + kcols, kcols)], wsem.at[2]),
    ]
    for c in w_copies:
        c.start()

    def in_copies(i):
        slot = lax.rem(i, DEPTH)
        rows = pl.ds(i * BLK, BLK)
        return (pltpu.make_async_copy(k_hbm.at[layer, rows], kbuf.at[slot], insem.at[0, slot]),
                pltpu.make_async_copy(v_hbm.at[layer, rows], vbuf.at[slot], insem.at[1, slot]))

    def out_copies(i):
        slot = lax.rem(i, DEPTH)
        rows = pl.ds(i * BLK, BLK)
        return (pltpu.make_async_copy(kbuf.at[slot], ko_hbm.at[layer, rows], outsem.at[0, slot]),
                pltpu.make_async_copy(vbuf.at[slot], vo_hbm.at[layer, rows], outsem.at[1, slot]))

    for i in range(DEPTH - LAG):
        for c in in_copies(i):
            c.start()

    h_buf[...] = normed(x_ref[...].astype(F32), norm_ref[layer:layer + 1, :].astype(F32))
    for c in w_copies:
        c.wait()

    @pl.loop(0, (qcols + 2 * kcols) // 256)
    def _(n):
        cols = pl.ds(pl.multiple_of(n * 256, 256), 256)
        qkv[n] = jnp.dot(h_buf[...], w_buf[:, cols], preferred_element_type=F32).astype(BF).astype(F32)

    cos_b = cos_ref[...]
    sin_b = sin_ref[...]

    def rope(vec):
        return (vec * cos_b + pltpu.roll(vec, 64, 1) * sin_b).astype(BF).astype(F32)

    zero = jnp.zeros((batch, 128), F32)
    for j in range(8):
        vec = rope(qkv[j // 2][:, (j % 2) * 128:(j % 2) * 128 + 128]) if j < heads else zero
        q_rows[pl.ds(j, batch, stride=8), :] = vec
    for h in range(2):
        k_vec = rope(qkv[heads // 2][:, h * 128:h * 128 + 128])
        v_vec = qkv[heads // 2 + 1][:, h * 128:h * 128 + 128]
        for r in range(4):
            k_rows[pl.ds(2 * r + h, batch, stride=8), :] = k_vec
            v_rows[pl.ds(2 * r + h, batch, stride=8), :] = v_vec

    col = lax.broadcasted_iota(jnp.int32, (8, 256), 1)
    row = lax.broadcasted_iota(jnp.int32, (8, 256), 0)
    own = (col & 1) == jnp.where(row >= heads // 2, 1, 0)
    key_row = jnp.where(own, col >> 1, 4096)
    seq_in_group = lax.broadcasted_iota(jnp.int32, (16, 128), 0) >> 1
    scale = 128 ** -0.5

    @pl.loop(0, nblk)
    def _(i):
        slot = lax.rem(i, DEPTH)
        for c in in_copies(i):
            c.wait()
        for b in range(BLK):
            pos = pos_ref[i * BLK + b]
            group = pl.ds(pl.multiple_of((pos >> 3) * 16, 16), 16)
            hit = seq_in_group == (pos & 7)
            rows = pl.ds(pl.multiple_of((i * BLK + b) * 8, 8), 8)
            for buf, new in ((kbuf, k_rows), (vbuf, v_rows)):
                new8 = new[rows, :]
                new16 = jnp.concatenate([new8, new8], axis=0)
                old16 = buf[slot, b, group, :].astype(F32)
                buf[slot, b, group, :] = jnp.where(hit, new16, old16).astype(BF)
        zero8 = jnp.zeros((8, 128), F32)
        for p in range(BLK // 2):
            first = i * BLK + 2 * p
            qa = q_rows[pl.ds(pl.multiple_of(first * 8, 8), 8), :]
            qb = q_rows[pl.ds(pl.multiple_of(first * 8 + 8, 8), 8), :]
            q2 = jnp.concatenate([jnp.concatenate([qa, zero8], axis=1), jnp.concatenate([zero8, qb], axis=1)], axis=0).astype(BF)
            k2 = jnp.concatenate([kbuf[slot, 2 * p], kbuf[slot, 2 * p + 1]], axis=1)
            v2 = jnp.concatenate([vbuf[slot, 2 * p], vbuf[slot, 2 * p + 1]], axis=1)
            s = lax.dot_general(q2, k2, (((1,), (1,)), ((), ())), preferred_element_type=F32) * scale
            keep = jnp.concatenate([key_row <= pos_ref[first], key_row <= pos_ref[first + 1]], axis=0)
            s = jnp.where(keep, s, NEG)
            e = jnp.exp(s - jnp.max(s, axis=-1, keepdims=True))
            w = (e * (1.0 / jnp.sum(e, axis=-1, keepdims=True))).astype(BF)
            o = jnp.dot(w, v2, preferred_element_type=F32)
            o_ref[pl.ds(pl.multiple_of(first * 8, 8), 8), :] = o[0:8, 0:128]
            o_ref[pl.ds(pl.multiple_of(first * 8 + 8, 8), 8), :] = o[8:16, 128:256]
        for c in out_copies(i):
            c.start()

        @pl.when(i >= LAG)
        def _():
            for c in out_copies(i - LAG):
                c.wait()

        @pl.when(i + DEPTH - LAG < nblk)
        def _():
            for c in in_copies(i + DEPTH - LAG):
                c.start()

    for i in range(nblk - LAG, nblk):
        for c in out_copies(i):
            c.wait()


def attention(layer, positions, hidden, norm, cos_f, sin_f, wq, wk, wv, k_cache, v_cache, prev):
    batch = hidden.shape[0]
    dim = hidden.shape[1]
    cols = wq.shape[2] + 2 * wk.shape[2]
    anyspec = pl.BlockSpec(memory_space=pl.ANY)
    vmem = pl.BlockSpec(memory_space=pltpu.VMEM)
    args = [positions, hidden, norm, cos_f, sin_f, wq, wk, wv, k_cache, v_cache]
    in_specs = [pl.BlockSpec(memory_space=pltpu.SMEM), vmem, vmem, vmem, vmem] + [anyspec] * 5
    aliases = {}
    if prev is not None:
        args += list(prev)
        in_specs += [anyspec] * 2
        aliases = {10: 1, 11: 2}
    return pl.pallas_call(
        functools.partial(attn_kernel, layer, prev is not None),
        out_shape=(jax.ShapeDtypeStruct((batch * 8, 128), F32),
                   jax.ShapeDtypeStruct(k_cache.shape, BF), jax.ShapeDtypeStruct(v_cache.shape, BF)),
        in_specs=in_specs,
        out_specs=(vmem, anyspec, anyspec),
        scratch_shapes=[
            pltpu.VMEM((dim, cols), BF),
            pltpu.VMEM((batch, dim), BF),
            pltpu.VMEM((cols // 256, batch, 256), F32),
            pltpu.VMEM((batch * 8, 128), F32),
            pltpu.VMEM((batch * 8, 128), F32),
            pltpu.VMEM((batch * 8, 128), F32),
            pltpu.VMEM((DEPTH, BLK, 256, 128), BF),
            pltpu.VMEM((DEPTH, BLK, 256, 128), BF),
            pltpu.SemaphoreType.DMA((3,)),
            pltpu.SemaphoreType.DMA((2, DEPTH)),
            pltpu.SemaphoreType.DMA((2, DEPTH)),
        ],
        input_output_aliases=aliases,
        compiler_params=pltpu.CompilerParams(vmem_limit_bytes=60 * 2**20),
        cost_estimate=pl.CostEstimate(flops=2 * batch * dim * cols, bytes_accessed=76 * 2**20, transcendentals=0),
        name=f"attn{layer}",
    )(*args)


CW = 512
HALF = 128


def mlp_kernel(layer, att_ref, x_ref, norm_ref, wo_hbm, wg_hbm, wu_hbm, wd_hbm, out_ref,
               wo, wg, wu, wd, att, h, act, own, sd, sx, sg, rd, rx, ra,
               wsem, sd_sem, sx_sem, sg_sem, rd_sem, rx_sem, ra_sem):
    dim = x_ref.shape[1]
    nch = dim // 2 // CW
    tp = lax.axis_index("tp")
    core = lax.rem(tp, 2)
    sib = tp + 1 - 2 * core
    peer = lax.rem(tp + 2, 4)
    mine = pl.multiple_of(core * (dim // 2), CW)
    theirs = pl.multiple_of((1 - core) * (dim // 2), CW)

    loads = []
    for idx, (src, dst) in enumerate(((wo_hbm, wo), (wg_hbm, wg), (wu_hbm, wu), (wd_hbm, wd))):
        loads.append(pltpu.make_async_copy(src.at[layer], dst, wsem.at[idx]))
    for c in loads:
        c.start()

    barrier = pltpu.get_barrier_semaphore()
    for other in (sib, peer):
        pl.semaphore_signal(barrier, inc=1, device_id={"tp": other}, device_id_type=MESH)
    pl.semaphore_wait(barrier, 2)

    out_ref[...] = x_ref[...]

    def to_sib(ph, k):
        return pltpu.make_async_remote_copy(sd.at[ph % 2, k], rd.at[ph, k], sd_sem.at[ph, k], rd_sem.at[ph, k],
                                            device_id={"tp": sib}, device_id_type=MESH)

    def to_peer(ph, k):
        return pltpu.make_async_remote_copy(sx.at[ph % 2, k], rx.at[ph, k], sx_sem.at[ph, k], rx_sem.at[ph, k],
                                            device_id={"tp": peer}, device_id_type=MESH)

    def share(ph, k):
        return pltpu.make_async_remote_copy(sg.at[ph % 2, k], ra.at[ph, k], sg_sem.at[ph, k], ra_sem.at[ph, k],
                                            device_id={"tp": sib}, device_id_type=MESH)

    def reduce_start(ph, lhs_ref, w_ref):
        for k in range(nch):
            sd[ph % 2, k] = jnp.dot(lhs_ref[...], w_ref[:, pl.ds(theirs + k * CW, CW)], preferred_element_type=F32).astype(BF)
            to_sib(ph, k).start()
        for k in range(nch):
            own[k] = jnp.dot(lhs_ref[...], w_ref[:, pl.ds(mine + k * CW, CW)], preferred_element_type=F32)
            to_sib(ph, k).wait_recv()
            sx[ph % 2, k] = (own[k] + rd[ph, k].astype(F32)).astype(BF)
            to_peer(ph, k).start()
        for k in range(nch):
            to_sib(ph, k).wait_send()

    def reduce_end(ph):
        rows = pl.ds((ph % 2) * HALF, HALF)
        for k in range(nch):
            to_peer(ph, k).wait()
            total = (sx[ph % 2, k].astype(F32) + rx[ph, k].astype(F32)).astype(BF)
            sg[ph % 2, k] = total
            share(ph, k).start()
            cols = pl.ds(mine + k * CW, CW)
            out_ref[rows, cols] = (out_ref[rows, cols].astype(F32) + total.astype(F32)).astype(BF)
        for k in range(nch):
            share(ph, k).wait()
            cols = pl.ds(theirs + k * CW, CW)
            out_ref[rows, cols] = (out_ref[rows, cols].astype(F32) + ra[ph, k].astype(F32)).astype(BF)

    def mlp(half):
        rows = pl.ds(half * HALF, HALF)
        h[...] = normed(out_ref[rows, :].astype(F32), norm_ref[layer:layer + 1, :].astype(F32))

        @pl.loop(0, act.shape[1] // 256)
        def _(n):
            cols = pl.ds(pl.multiple_of(n * 256, 256), 256)
            g = jnp.dot(h[...], wg[:, cols], preferred_element_type=F32).astype(BF).astype(F32)
            u = jnp.dot(h[...], wu[:, cols], preferred_element_type=F32).astype(BF).astype(F32)
            act[:, cols] = (g * jax.nn.sigmoid(g) * u).astype(BF)

    loads[0].wait()
    for half in range(2):
        for j in range(att.shape[1] // 128):
            att[:, j * 128:(j + 1) * 128] = att_ref[pl.ds(half * HALF * 8 + j, HALF, stride=8), :].astype(BF)
        reduce_start(half, att, wo)
    for half in range(2):
        reduce_end(half)
        if half == 0:
            loads[1].wait()
            loads[2].wait()
        mlp(half)
        if half == 0:
            loads[3].wait()
        reduce_start(2 + half, act, wd)
    for half in range(2):
        reduce_end(2 + half)


def mlp_block(layer, att, hidden, norm, wo, wg, wu, wd):
    batch, dim = hidden.shape
    nch = dim // 2 // CW
    anyspec = pl.BlockSpec(memory_space=pl.ANY)
    vmem = pl.BlockSpec(memory_space=pltpu.VMEM)
    msg = lambda n: pltpu.VMEM((n, nch, HALF, CW), BF)
    sems = pltpu.SemaphoreType.DMA((4, nch))
    return pl.pallas_call(
        functools.partial(mlp_kernel, layer),
        out_shape=jax.ShapeDtypeStruct((batch, dim), BF),
        in_specs=[vmem, vmem, vmem] + [anyspec] * 4,
        out_specs=vmem,
        scratch_shapes=[
            pltpu.VMEM(wo.shape[1:], BF), pltpu.VMEM(wg.shape[1:], BF), pltpu.VMEM(wu.shape[1:], BF), pltpu.VMEM(wd.shape[1:], BF),
            pltpu.VMEM((HALF, wo.shape[1]), BF), pltpu.VMEM((HALF, dim), BF), pltpu.VMEM((HALF, wd.shape[1]), BF),
            pltpu.VMEM((nch, HALF, CW), F32),
            msg(2), msg(2), msg(2), msg(4), msg(4), msg(4),
            pltpu.SemaphoreType.DMA((4,)), sems, sems, sems, sems, sems, sems,
        ],
        compiler_params=pltpu.CompilerParams(collective_id=layer, has_side_effects=True, vmem_limit_bytes=62 * 2**20),
        name=f"mlp{layer}",
    )(att, hidden, norm, wo, wg, wu, wd)


def solution(mesh):
    row_spec = P('dp', None)
    pos_spec = P('dp')
    cache_spec = P(None, 'dp', None, 'tp', None)
    norm_spec = P(None, None)
    col_spec = P(None, None, 'tp')
    split_rows = P(None, 'tp', None)

    def local_step(hidden, positions, k_cache, v_cache, attn_norm, w_query, w_key, w_value, w_out, mlp_norm, w_gate, w_up, w_down):
        cache_shape = k_cache.shape
        flat = (cache_shape[0], cache_shape[1], cache_shape[2] * cache_shape[3], cache_shape[4])
        k_flat, v_flat = k_cache.reshape(flat), v_cache.reshape(flat)
        cos_f, sin_f = rope_full(positions, cache_shape[4])
        caches = None
        for layer in range(cache_shape[0]):
            att, *caches = attention(layer, positions, hidden, attn_norm, cos_f, sin_f, w_query, w_key, w_value, k_flat, v_flat, caches)
            hidden = mlp_block(layer, att, hidden, mlp_norm, w_out, w_gate, w_up, w_down)
        return hidden, caches[0].reshape(cache_shape), caches[1].reshape(cache_shape)

    return jax.shard_map(local_step, mesh=mesh, in_specs=(row_spec, pos_spec, cache_spec, cache_spec, norm_spec, col_spec, col_spec, col_spec, split_rows, norm_spec, col_spec, col_spec, split_rows), out_specs=(row_spec, cache_spec, cache_spec), check_vma=False)
```

```python
import functools
import math
import jax
import jax.numpy as jnp
import numpy as np
from jax import lax
from jax.experimental import pallas as pl
from jax.experimental.pallas import tpu as pltpu
from jax.sharding import PartitionSpec as P

BF = jnp.bfloat16
F32 = jnp.float32
MESH = pl.DeviceIdType.MESH
EPS = 1e-5
NEG = -1e30


def rope_table(rows, head_dim):
    half_dim = head_dim // 2
    inv_freq = np.power(np.float32(500000.0), -np.arange(half_dim, dtype=np.float32) * np.float32(2.0 / head_dim)).astype(np.float32)
    wavelen = (np.float32(2.0 * math.pi) / inv_freq).astype(np.float32)
    smooth = (np.float32(8192.0) / wavelen - np.float32(1.0)) / np.float32(3.0)
    blended = (np.float32(1.0) - smooth) * inv_freq / np.float32(8.0) + smooth * inv_freq
    scaled = np.where(wavelen < 2048.0, inv_freq, np.where(wavelen > 8192.0, inv_freq / np.float32(8.0), blended)).astype(np.float32)
    angles = np.arange(rows, dtype=np.float32)[:, None] * scaled[None, :]
    cos, sin = np.cos(angles.astype(np.float64)), np.sin(angles.astype(np.float64))
    return np.concatenate([cos, cos, -sin, sin], axis=-1).astype(np.float32)


def normed(x_f32, weight_f32):
    mean_sq = jnp.mean(x_f32 * x_f32, axis=-1, keepdims=True)
    return (x_f32 * lax.rsqrt(mean_sq + EPS) * weight_f32).astype(BF)


BLK = 16


def attn_kernel(layer, has_qkv, aliased, *refs):
    pos_hbm, table_hbm = refs[:2]
    if has_qkv:
        qkv_hbm, k_hbm, v_hbm = refs[2:5]
        refs = refs[5:]
    else:
        x_hbm, norm_hbm, wq_hbm, wk_hbm, wv_hbm, k_hbm, v_hbm = refs[2:9]
        refs = refs[9:]
    if aliased:
        refs = refs[2:]
    att_hbm, ko_hbm, vo_hbm, pos_ref, table, qkv, cs, q_rows, k_rows, v_rows, o_rows, att, kbuf, vbuf, sem, insem, outsem, *rest = refs
    nblk = kbuf.shape[0]
    batch = nblk * BLK
    heads = att.shape[1] // 128

    pos_copy = pltpu.make_async_copy(pos_hbm, pos_ref, sem.at[0])
    table_copy = pltpu.make_async_copy(table_hbm, table, sem.at[1])
    pos_copy.start()
    table_copy.start()
    if has_qkv:
        first = [pltpu.make_async_copy(qkv_hbm, qkv, sem.at[2])]
    else:
        x_buf, norm, w_buf, h_buf = rest
        qcols = wq_hbm.shape[2]
        kcols = wk_hbm.shape[2]
        x_copies = [pltpu.make_async_copy(x_hbm, x_buf, sem.at[3]), pltpu.make_async_copy(norm_hbm, norm, sem.at[4])]
        for c in x_copies:
            c.start()
        first = [
            pltpu.make_async_copy(wq_hbm.at[layer], w_buf.at[:, pl.ds(0, qcols)], sem.at[5]),
            pltpu.make_async_copy(wk_hbm.at[layer], w_buf.at[:, pl.ds(qcols, kcols)], sem.at[6]),
            pltpu.make_async_copy(wv_hbm.at[layer], w_buf.at[:, pl.ds(qcols + kcols, kcols)], sem.at[7]),
        ]
    for c in first:
        c.start()

    def in_copies(i):
        rows = pl.ds(i * BLK, BLK)
        return (pltpu.make_async_copy(k_hbm.at[layer, rows], kbuf.at[i], insem.at[0, i]),
                pltpu.make_async_copy(v_hbm.at[layer, rows], vbuf.at[i], insem.at[1, i]))

    def out_copies(i):
        rows = pl.ds(i * BLK, BLK)
        return (pltpu.make_async_copy(kbuf.at[i], ko_hbm.at[layer, rows], outsem.at[0, i]),
                pltpu.make_async_copy(vbuf.at[i], vo_hbm.at[layer, rows], outsem.at[1, i]))

    @pl.loop(0, nblk)
    def _(i):
        for c in in_copies(i):
            c.start()

    pos_copy.wait()
    table_copy.wait()

    @pl.loop(0, batch // 8)
    def _(i):
        for b in range(8):
            r = i * 8 + b
            cs[pl.ds(r, 1), :] = table[pl.ds(pos_ref[r], 1), :]

    if not has_qkv:
        for c in x_copies:
            c.wait()
        h_buf[...] = normed(x_buf[...].astype(F32), norm[layer:layer + 1, :].astype(F32))
    for c in first:
        c.wait()
    if not has_qkv:
        @pl.loop(0, (qcols + 2 * kcols) // 256)
        def _(n):
            cols = pl.ds(pl.multiple_of(n * 256, 256), 256)
            qkv[n] = jnp.dot(h_buf[...], w_buf[:, cols], preferred_element_type=F32).astype(BF)

    cos_b = cs[:, 0:128]
    sin_b = cs[:, 128:256]

    def piece(n, h):
        return qkv[n, :, h * 128:h * 128 + 128].astype(F32)

    def rope(vec):
        return (vec * cos_b + pltpu.roll(vec, 64, 1) * sin_b).astype(BF).astype(F32)

    zero = jnp.zeros((batch, 128), F32)
    for j in range(8):
        q_rows[pl.ds(j, batch, stride=8), :] = rope(piece(j // 2, j % 2)) if j < heads else zero
    for h in range(2):
        k_vec = rope(piece(heads // 2, h))
        v_vec = piece(heads // 2 + 1, h)
        for r in range(4):
            k_rows[pl.ds(2 * r + h, batch, stride=8), :] = k_vec
            v_rows[pl.ds(2 * r + h, batch, stride=8), :] = v_vec

    col = lax.broadcasted_iota(jnp.int32, (8, 256), 1)
    row = lax.broadcasted_iota(jnp.int32, (8, 256), 0)
    own = (col & 1) == jnp.where(row >= heads // 2, 1, 0)
    key_row = jnp.where(own, col >> 1, 4096)
    seq_in_group = lax.broadcasted_iota(jnp.int32, (16, 128), 0) >> 1
    scale = 128 ** -0.5

    @pl.loop(0, nblk)
    def _(i):
        for c in in_copies(i):
            c.wait()
        for b in range(BLK):
            pos = pos_ref[i * BLK + b]
            group = pl.ds(pl.multiple_of((pos >> 3) * 16, 16), 16)
            hit = seq_in_group == (pos & 7)
            rows = pl.ds(pl.multiple_of((i * BLK + b) * 8, 8), 8)
            for buf, new in ((kbuf, k_rows), (vbuf, v_rows)):
                new8 = new[rows, :]
                new16 = jnp.concatenate([new8, new8], axis=0)
                old16 = buf[i, b, group, :].astype(F32)
                buf[i, b, group, :] = jnp.where(hit, new16, old16).astype(BF)
        zero8 = jnp.zeros((8, 128), F32)
        pairs = range(BLK // 2)
        scores = []
        for p in pairs:
            first = i * BLK + 2 * p
            qa = q_rows[pl.ds(pl.multiple_of(first * 8, 8), 8), :]
            qb = q_rows[pl.ds(pl.multiple_of(first * 8 + 8, 8), 8), :]
            q2 = jnp.concatenate([jnp.concatenate([qa, zero8], axis=1), jnp.concatenate([zero8, qb], axis=1)], axis=0).astype(BF)
            k2 = jnp.concatenate([kbuf[i, 2 * p], kbuf[i, 2 * p + 1]], axis=1)
            scores.append(lax.dot_general(q2, k2, (((1,), (1,)), ((), ())), preferred_element_type=F32))
        weights = []
        for p in pairs:
            first = i * BLK + 2 * p
            keep = jnp.concatenate([key_row <= pos_ref[first], key_row <= pos_ref[first + 1]], axis=0)
            s = jnp.where(keep, scores[p] * scale, NEG)
            e = jnp.exp(s - jnp.max(s, axis=-1, keepdims=True))
            weights.append((e * (1.0 / jnp.sum(e, axis=-1, keepdims=True))).astype(BF))
        outs = []
        for p in pairs:
            v2 = jnp.concatenate([vbuf[i, 2 * p], vbuf[i, 2 * p + 1]], axis=1)
            outs.append(jnp.dot(weights[p], v2, preferred_element_type=F32))
        for c in out_copies(i):
            c.start()
        for p in pairs:
            o_rows[16 * p:16 * p + 8, :] = outs[p][0:8, 0:128]
            o_rows[16 * p + 8:16 * p + 16, :] = outs[p][8:16, 128:256]
        rows = pl.ds(pl.multiple_of(i * BLK, BLK), BLK)
        for j in range(heads):
            att[rows, j * 128:(j + 1) * 128] = o_rows[pl.ds(j, BLK, stride=8), :].astype(BF)

    att_copy = pltpu.make_async_copy(att, att_hbm, sem.at[8])
    att_copy.start()
    att_copy.wait()

    @pl.loop(0, nblk)
    def _(i):
        for c in out_copies(i):
            c.wait()


def attention(layer, positions, table, source, k_cache, v_cache, prev, qcols, kcols):
    batch = positions.shape[0]
    has_qkv = len(source) == 1
    anyspec = pl.BlockSpec(memory_space=pl.ANY)
    args = [positions, table, *source, k_cache, v_cache]
    aliases = {}
    if prev is not None:
        aliases = {len(args): 1, len(args) + 1: 2}
        args += list(prev)
    cols = qcols + 2 * kcols
    nblk = batch // BLK
    scratch = [
        pltpu.SMEM((batch,), jnp.int32),
        pltpu.VMEM(table.shape, F32),
        pltpu.VMEM((cols // 256, batch, 256), BF),
        pltpu.VMEM((batch, table.shape[1]), F32),
        pltpu.VMEM((batch * 8, 128), F32),
        pltpu.VMEM((batch * 8, 128), F32),
        pltpu.VMEM((batch * 8, 128), F32),
        pltpu.VMEM((BLK * 8, 128), F32),
        pltpu.VMEM((batch, qcols), BF),
        pltpu.VMEM((nblk, BLK) + k_cache.shape[2:], BF),
        pltpu.VMEM((nblk, BLK) + v_cache.shape[2:], BF),
        pltpu.SemaphoreType.DMA((9,)),
        pltpu.SemaphoreType.DMA((2, nblk)),
        pltpu.SemaphoreType.DMA((2, nblk)),
    ]
    if not has_qkv:
        hidden, norm = source[:2]
        dim = hidden.shape[1]
        scratch += [pltpu.VMEM(hidden.shape, BF), pltpu.VMEM(norm.shape, BF), pltpu.VMEM((dim, cols), BF), pltpu.VMEM(hidden.shape, BF)]
    return pl.pallas_call(
        functools.partial(attn_kernel, layer, has_qkv, prev is not None),
        out_shape=(jax.ShapeDtypeStruct((batch, qcols), BF),
                   jax.ShapeDtypeStruct(k_cache.shape, BF), jax.ShapeDtypeStruct(v_cache.shape, BF)),
        in_specs=[anyspec] * len(args),
        out_specs=(anyspec, anyspec, anyspec),
        scratch_shapes=scratch,
        input_output_aliases=aliases,
        compiler_params=pltpu.CompilerParams(vmem_limit_bytes=62 * 2**20),
        cost_estimate=pl.CostEstimate(flops=2 * batch * 3072 * cols, bytes_accessed=76 * 2**20, transcendentals=0),
        name=f"attn{layer}",
    )(*args)


CW = 512
HALF = 128
GW = 512


def mlp_kernel(layer, next_qkv, att_hbm, x_hbm, norm_hbm, wo_hbm, wg_hbm, wu_hbm, wd_hbm, *refs):
    if next_qkv:
        norm2_hbm, wq_hbm, wk_hbm, wv_hbm, out_hbm, qkv_hbm = refs[:6]
        refs = refs[6:]
    else:
        out_hbm = refs[0]
        refs = refs[1:]
    (wo, wg, wu, wd, att, x, norm, h, act, sd, sx, sg, rd, rx, ra,
     wsem, isem, sd_sem, sx_sem, sg_sem, rd_sem, rx_sem, ra_sem, *refs) = refs
    dim = x.shape[1]
    nch = dim // 2 // CW
    tp = lax.axis_index("tp")
    core = lax.rem(tp, 2)
    sib = tp + 1 - 2 * core
    peer = lax.rem(tp + 2, 4)
    mine = pl.multiple_of(core * (dim // 2), CW)
    theirs = pl.multiple_of((1 - core) * (dim // 2), CW)

    half_rows = wo.shape[0] // 2
    att_copy = pltpu.make_async_copy(att_hbm, att, isem.at[0])
    wo_copies = [pltpu.make_async_copy(wo_hbm.at[layer, pl.ds(r * half_rows, half_rows)], wo.at[pl.ds(r * half_rows, half_rows)], wsem.at[r]) for r in range(2)]
    x_copy = pltpu.make_async_copy(x_hbm, x, isem.at[1])
    norm_copy = pltpu.make_async_copy(norm_hbm, norm, isem.at[2])
    wg_copy = pltpu.make_async_copy(wg_hbm.at[layer], wg, wsem.at[2])
    wu_copy = pltpu.make_async_copy(wu_hbm.at[layer], wu, wsem.at[3])
    wd_copy = pltpu.make_async_copy(wd_hbm.at[layer], wd, wsem.at[4])
    for c in [att_copy, *wo_copies]:
        c.start()
    if next_qkv:
        norm2, wqkv, qkv = refs
        qcols = wq_hbm.shape[2]
        kcols = wk_hbm.shape[2]
        qkv_loads = [
            pltpu.make_async_copy(norm2_hbm, norm2, isem.at[3]),
            pltpu.make_async_copy(wq_hbm.at[layer + 1], wqkv.at[:, pl.ds(0, qcols)], wsem.at[5]),
            pltpu.make_async_copy(wk_hbm.at[layer + 1], wqkv.at[:, pl.ds(qcols, kcols)], wsem.at[6]),
            pltpu.make_async_copy(wv_hbm.at[layer + 1], wqkv.at[:, pl.ds(qcols + kcols, kcols)], wsem.at[7]),
        ]

    barrier = pltpu.get_barrier_semaphore()
    for other in (sib, peer):
        pl.semaphore_signal(barrier, inc=1, device_id={"tp": other}, device_id_type=MESH)
    pl.semaphore_wait(barrier, 2)

    def to_sib(ph, k):
        return pltpu.make_async_remote_copy(sd.at[ph % 2, k], rd.at[ph, k], sd_sem.at[ph, k], rd_sem.at[ph, k],
                                            device_id={"tp": sib}, device_id_type=MESH)

    def to_peer(ph, k):
        return pltpu.make_async_remote_copy(sx.at[ph % 2, k], rx.at[ph, k], sx_sem.at[ph, k], rx_sem.at[ph, k],
                                            device_id={"tp": peer}, device_id_type=MESH)

    def share(ph, k):
        return pltpu.make_async_remote_copy(sg.at[ph % 2, k], ra.at[ph, k], sg_sem.at[ph, k], ra_sem.at[ph, k],
                                            device_id={"tp": sib}, device_id_type=MESH)

    def reduce_start(ph, lhs, w_ref):
        for k in range(nch):
            sd[ph % 2, k] = jnp.dot(lhs, w_ref[:, pl.ds(theirs + k * CW, CW)], preferred_element_type=F32).astype(BF)
            to_sib(ph, k).start()
        for k in range(nch):
            part = jnp.dot(lhs, w_ref[:, pl.ds(mine + k * CW, CW)], preferred_element_type=F32)
            to_sib(ph, k).wait_recv()
            sx[ph % 2, k] = (part + rd[ph, k].astype(F32)).astype(BF)
            to_peer(ph, k).start()
        for k in range(nch):
            to_sib(ph, k).wait_send()

    def reduce_end(ph):
        rows = pl.ds((ph % 2) * HALF, HALF)
        for k in range(nch):
            to_peer(ph, k).wait()
            total = (sx[ph % 2, k].astype(F32) + rx[ph, k].astype(F32)).astype(BF)
            sg[ph % 2, k] = total
            share(ph, k).start()
            cols = pl.ds(mine + k * CW, CW)
            x[rows, cols] = (x[rows, cols].astype(F32) + total.astype(F32)).astype(BF)
        for k in range(nch):
            share(ph, k).wait()
            cols = pl.ds(theirs + k * CW, CW)
            x[rows, cols] = (x[rows, cols].astype(F32) + ra[ph, k].astype(F32)).astype(BF)

    def mlp(half):
        rows = pl.ds(half * HALF, HALF)
        h[...] = normed(x[rows, :].astype(F32), norm[layer:layer + 1, :].astype(F32))

        @pl.loop(0, act.shape[1] // GW)
        def _(n):
            cols = pl.ds(pl.multiple_of(n * GW, GW), GW)
            g = jnp.dot(h[...], wg[:, cols], preferred_element_type=F32).astype(BF).astype(F32)
            u = jnp.dot(h[...], wu[:, cols], preferred_element_type=F32).astype(BF).astype(F32)
            act[:, cols] = (g * jax.nn.sigmoid(g) * u).astype(BF)

    def out_copy(half):
        rows = pl.ds(half * HALF, HALF)
        return pltpu.make_async_copy(x.at[rows], out_hbm.at[rows], isem.at[4 + half])

    def qkv_copy(half):
        rows = pl.ds(half * HALF, HALF)
        return pltpu.make_async_copy(qkv.at[:, rows], qkv_hbm.at[:, rows], isem.at[6 + half])

    att_copy.wait()
    for c in wo_copies:
        c.wait()
    for c in (x_copy, norm_copy, wg_copy, wu_copy):
        c.start()
    for half in range(2):
        reduce_start(half, att[half * HALF:(half + 1) * HALF, :], wo)
    wd_copy.start()
    if next_qkv:
        for c in qkv_loads:
            c.start()
    x_copy.wait()
    norm_copy.wait()
    for half in range(2):
        reduce_end(half)
        if half == 0:
            wg_copy.wait()
            wu_copy.wait()
        mlp(half)
        if half == 0:
            wd_copy.wait()
        reduce_start(2 + half, act[...], wd)
    if next_qkv:
        for c in qkv_loads:
            c.wait()
    for half in range(2):
        rows = pl.ds(half * HALF, HALF)
        reduce_end(2 + half)
        out_copy(half).start()
        if next_qkv:
            h[...] = normed(x[rows, :].astype(F32), norm2[layer + 1:layer + 2, :].astype(F32))

            @pl.loop(0, qkv.shape[0])
            def _(n):
                cols = pl.ds(pl.multiple_of(n * 256, 256), 256)
                qkv[n, rows, :] = jnp.dot(h[...], wqkv[:, cols], preferred_element_type=F32).astype(BF)

            qkv_copy(half).start()
    for half in range(2):
        out_copy(half).wait()
        if next_qkv:
            qkv_copy(half).wait()


def mlp_block(layer, att, hidden, norm, wo, wg, wu, wd, following):
    batch, dim = hidden.shape
    nch = dim // 2 // CW
    anyspec = pl.BlockSpec(memory_space=pl.ANY)
    msg = lambda n: pltpu.VMEM((n, nch, HALF, CW), BF)
    sems = pltpu.SemaphoreType.DMA((4, nch))
    args = [att, hidden, norm, wo, wg, wu, wd]
    scratch = [
        pltpu.VMEM(wo.shape[1:], BF), pltpu.VMEM(wg.shape[1:], BF), pltpu.VMEM(wu.shape[1:], BF), pltpu.VMEM(wd.shape[1:], BF),
        pltpu.VMEM(att.shape, BF), pltpu.VMEM(hidden.shape, BF), pltpu.VMEM(norm.shape, BF),
        pltpu.VMEM((HALF, dim), BF), pltpu.VMEM((HALF, wd.shape[1]), BF),
        msg(2), msg(2), msg(2), msg(4), msg(4), msg(4),
        pltpu.SemaphoreType.DMA((8,)), pltpu.SemaphoreType.DMA((8,)), sems, sems, sems, sems, sems, sems,
    ]
    out_shape = [jax.ShapeDtypeStruct((batch, dim), BF)]
    if following is not None:
        norm2, wq, wk, wv = following
        args += list(following)
        cols = wq.shape[2] + 2 * wk.shape[2]
        out_shape.append(jax.ShapeDtypeStruct((cols // 256, batch, 256), BF))
        scratch += [pltpu.VMEM(norm2.shape, BF), pltpu.VMEM((dim, cols), BF), pltpu.VMEM((cols // 256, batch, 256), BF)]
    return pl.pallas_call(
        functools.partial(mlp_kernel, layer, following is not None),
        out_shape=out_shape,
        in_specs=[anyspec] * len(args),
        out_specs=[anyspec] * len(out_shape),
        scratch_shapes=scratch,
        compiler_params=pltpu.CompilerParams(collective_id=layer, has_side_effects=True, vmem_limit_bytes=67043328),
        name=f"mlp{layer}",
    )(*args)


def solution(mesh):
    row_spec = P('dp', None)
    pos_spec = P('dp')
    cache_spec = P(None, 'dp', None, 'tp', None)
    norm_spec = P(None, None)
    col_spec = P(None, None, 'tp')
    split_rows = P(None, 'tp', None)

    def local_step(hidden, positions, k_cache, v_cache, attn_norm, w_query, w_key, w_value, w_out, mlp_norm, w_gate, w_up, w_down):
        cache_shape = k_cache.shape
        flat = (cache_shape[0], cache_shape[1], cache_shape[2] * cache_shape[3], cache_shape[4])
        k_flat, v_flat = k_cache.reshape(flat), v_cache.reshape(flat)
        table = jnp.asarray(rope_table(cache_shape[2], cache_shape[4]))
        layers = cache_shape[0]
        caches = None
        source = (hidden, attn_norm, w_query, w_key, w_value)
        for layer in range(layers):
            att, *caches = attention(layer, positions, table, source, k_flat, v_flat, caches, w_query.shape[2], w_key.shape[2])
            following = (attn_norm, w_query, w_key, w_value) if layer + 1 < layers else None
            hidden, *source = mlp_block(layer, att, hidden, mlp_norm, w_out, w_gate, w_up, w_down, following)
        return hidden, caches[0].reshape(cache_shape), caches[1].reshape(cache_shape)

    return jax.shard_map(local_step, mesh=mesh, in_specs=(row_spec, pos_spec, cache_spec, cache_spec, norm_spec, col_spec, col_spec, col_spec, split_rows, norm_spec, col_spec, col_spec, split_rows), out_specs=(row_spec, cache_spec, cache_spec), check_vma=False)
```

```python
import functools
import math
import jax
import jax.numpy as jnp
import numpy as np
from jax import lax
from jax.experimental import pallas as pl
from jax.experimental.pallas import tpu as pltpu
from jax.sharding import PartitionSpec as P

BF = jnp.bfloat16
F32 = jnp.float32
MESH = pl.DeviceIdType.MESH
EPS = 1e-5
NEG = -1e30


def rope_table(rows, head_dim):
    half_dim = head_dim // 2
    inv_freq = np.power(np.float32(500000.0), -np.arange(half_dim, dtype=np.float32) * np.float32(2.0 / head_dim)).astype(np.float32)
    wavelen = (np.float32(2.0 * math.pi) / inv_freq).astype(np.float32)
    smooth = (np.float32(8192.0) / wavelen - np.float32(1.0)) / np.float32(3.0)
    blended = (np.float32(1.0) - smooth) * inv_freq / np.float32(8.0) + smooth * inv_freq
    scaled = np.where(wavelen < 2048.0, inv_freq, np.where(wavelen > 8192.0, inv_freq / np.float32(8.0), blended)).astype(np.float32)
    angles = np.arange(rows, dtype=np.float32)[:, None] * scaled[None, :]
    cos, sin = np.cos(angles.astype(np.float64)), np.sin(angles.astype(np.float64))
    return np.concatenate([cos, cos, -sin, sin], axis=-1).astype(np.float32)


def normed(x_f32, weight_f32):
    mean_sq = jnp.mean(x_f32 * x_f32, axis=-1, keepdims=True)
    return (x_f32 * lax.rsqrt(mean_sq + EPS) * weight_f32).astype(BF)


BLK = 16
HOLD = 4


def attn_kernel(layer, has_qkv, aliased, *refs):
    pos_hbm, table_hbm = refs[:2]
    if has_qkv:
        qkv_hbm, k_hbm, v_hbm = refs[2:5]
        refs = refs[5:]
    else:
        x_hbm, norm_hbm, wq_hbm, wk_hbm, wv_hbm, k_hbm, v_hbm = refs[2:9]
        refs = refs[9:]
    if aliased:
        refs = refs[2:]
    att_hbm, ko_hbm, vo_hbm, pos_ref, table, qkv, cs, q_rows, k_rows, v_rows, o_rows, att, kbuf, vbuf, sem, insem, outsem, *rest = refs
    nblk = kbuf.shape[0]
    batch = nblk * BLK
    heads = att.shape[1] // 128

    pos_copy = pltpu.make_async_copy(pos_hbm, pos_ref, sem.at[0])
    table_copy = pltpu.make_async_copy(table_hbm, table, sem.at[1])
    pos_copy.start()
    table_copy.start()
    if has_qkv:
        first = [pltpu.make_async_copy(qkv_hbm, qkv, sem.at[2])]
    else:
        x_buf, norm, w_buf, h_buf = rest
        qcols = wq_hbm.shape[2]
        kcols = wk_hbm.shape[2]
        x_copies = [pltpu.make_async_copy(x_hbm, x_buf, sem.at[3]), pltpu.make_async_copy(norm_hbm, norm, sem.at[4])]
        for c in x_copies:
            c.start()
        first = [
            pltpu.make_async_copy(wq_hbm.at[layer], w_buf.at[:, pl.ds(0, qcols)], sem.at[5]),
            pltpu.make_async_copy(wk_hbm.at[layer], w_buf.at[:, pl.ds(qcols, kcols)], sem.at[6]),
            pltpu.make_async_copy(wv_hbm.at[layer], w_buf.at[:, pl.ds(qcols + kcols, kcols)], sem.at[7]),
        ]
    for c in first:
        c.start()

    def in_copies(i):
        rows = pl.ds(i * BLK, BLK)
        return (pltpu.make_async_copy(k_hbm.at[layer, rows], kbuf.at[i], insem.at[0, i]),
                pltpu.make_async_copy(v_hbm.at[layer, rows], vbuf.at[i], insem.at[1, i]))

    def out_copies(i):
        rows = pl.ds(i * BLK, BLK)
        return (pltpu.make_async_copy(kbuf.at[i], ko_hbm.at[layer, rows], outsem.at[0, i]),
                pltpu.make_async_copy(vbuf.at[i], vo_hbm.at[layer, rows], outsem.at[1, i]))

    @pl.loop(0, nblk)
    def _(i):
        for c in in_copies(i):
            c.start()

    pos_copy.wait()
    table_copy.wait()

    @pl.loop(0, batch // 8)
    def _(i):
        for b in range(8):
            r = i * 8 + b
            cs[pl.ds(r, 1), :] = table[pl.ds(pos_ref[r], 1), :]

    if not has_qkv:
        for c in x_copies:
            c.wait()
        h_buf[...] = normed(x_buf[...].astype(F32), norm[layer:layer + 1, :].astype(F32))
    for c in first:
        c.wait()
    if not has_qkv:
        @pl.loop(0, (qcols + 2 * kcols) // 256)
        def _(n):
            cols = pl.ds(pl.multiple_of(n * 256, 256), 256)
            qkv[n] = jnp.dot(h_buf[...], w_buf[:, cols], preferred_element_type=F32).astype(BF)

    cos_b = cs[:, 0:128]
    sin_b = cs[:, 128:256]

    def piece(n, h):
        return qkv[n, :, h * 128:h * 128 + 128].astype(F32)

    def rope(vec):
        return (vec * cos_b + pltpu.roll(vec, 64, 1) * sin_b).astype(BF).astype(F32)

    zero = jnp.zeros((batch, 128), F32)
    for j in range(8):
        q_rows[pl.ds(j, batch, stride=8), :] = rope(piece(j // 2, j % 2)) if j < heads else zero
    for h in range(2):
        k_vec = rope(piece(heads // 2, h))
        v_vec = piece(heads // 2 + 1, h)
        for r in range(4):
            k_rows[pl.ds(2 * r + h, batch, stride=8), :] = k_vec
            v_rows[pl.ds(2 * r + h, batch, stride=8), :] = v_vec

    col = lax.broadcasted_iota(jnp.int32, (8, 256), 1)
    row = lax.broadcasted_iota(jnp.int32, (8, 256), 0)
    own = (col & 1) == jnp.where(row >= heads // 2, 1, 0)
    key_row = jnp.where(own, col >> 1, 4096)
    seq_in_group = lax.broadcasted_iota(jnp.int32, (16, 128), 0) >> 1
    scale = 128 ** -0.5

    @pl.loop(0, nblk)
    def _(i):
        for c in in_copies(i):
            c.wait()
        for b in range(BLK):
            pos = pos_ref[i * BLK + b]
            group = pl.ds(pl.multiple_of((pos >> 3) * 16, 16), 16)
            hit = seq_in_group == (pos & 7)
            rows = pl.ds(pl.multiple_of((i * BLK + b) * 8, 8), 8)
            for buf, new in ((kbuf, k_rows), (vbuf, v_rows)):
                new8 = new[rows, :]
                new16 = jnp.concatenate([new8, new8], axis=0)
                old16 = buf[i, b, group, :].astype(F32)
                buf[i, b, group, :] = jnp.where(hit, new16, old16).astype(BF)
        zero8 = jnp.zeros((8, 128), F32)
        pairs = range(BLK // 2)
        scores = []
        for p in pairs:
            first = i * BLK + 2 * p
            qa = q_rows[pl.ds(pl.multiple_of(first * 8, 8), 8), :]
            qb = q_rows[pl.ds(pl.multiple_of(first * 8 + 8, 8), 8), :]
            q2 = jnp.concatenate([jnp.concatenate([qa, zero8], axis=1), jnp.concatenate([zero8, qb], axis=1)], axis=0).astype(BF)
            k2 = jnp.concatenate([kbuf[i, 2 * p], kbuf[i, 2 * p + 1]], axis=1)
            scores.append(lax.dot_general(q2, k2, (((1,), (1,)), ((), ())), preferred_element_type=F32))
        weights = []
        for p in pairs:
            first = i * BLK + 2 * p
            keep = jnp.concatenate([key_row <= pos_ref[first], key_row <= pos_ref[first + 1]], axis=0)
            s = jnp.where(keep, scores[p] * scale, NEG)
            e = jnp.exp(s - jnp.max(s, axis=-1, keepdims=True))
            weights.append((e * (1.0 / jnp.sum(e, axis=-1, keepdims=True))).astype(BF))
        outs = []
        for p in pairs:
            v2 = jnp.concatenate([vbuf[i, 2 * p], vbuf[i, 2 * p + 1]], axis=1)
            outs.append(jnp.dot(weights[p], v2, preferred_element_type=F32))

        @pl.when(i == HOLD)
        def _():
            @pl.loop(0, HOLD)
            def _(j):
                for c in out_copies(j):
                    c.start()

        @pl.when(i >= HOLD)
        def _():
            for c in out_copies(i):
                c.start()

        for p in pairs:
            o_rows[16 * p:16 * p + 8, :] = outs[p][0:8, 0:128]
            o_rows[16 * p + 8:16 * p + 16, :] = outs[p][8:16, 128:256]
        rows = pl.ds(pl.multiple_of(i * BLK, BLK), BLK)
        for j in range(heads):
            att[rows, j * 128:(j + 1) * 128] = o_rows[pl.ds(j, BLK, stride=8), :].astype(BF)

    att_copy = pltpu.make_async_copy(att, att_hbm, sem.at[8])
    att_copy.start()
    att_copy.wait()

    @pl.loop(0, nblk)
    def _(i):
        for c in out_copies(i):
            c.wait()


def attention(layer, positions, table, source, k_cache, v_cache, prev, qcols, kcols):
    batch = positions.shape[0]
    has_qkv = len(source) == 1
    anyspec = pl.BlockSpec(memory_space=pl.ANY)
    args = [positions, table, *source, k_cache, v_cache]
    aliases = {}
    if prev is not None:
        aliases = {len(args): 1, len(args) + 1: 2}
        args += list(prev)
    cols = qcols + 2 * kcols
    nblk = batch // BLK
    scratch = [
        pltpu.SMEM((batch,), jnp.int32),
        pltpu.VMEM(table.shape, F32),
        pltpu.VMEM((cols // 256, batch, 256), BF),
        pltpu.VMEM((batch, table.shape[1]), F32),
        pltpu.VMEM((batch * 8, 128), F32),
        pltpu.VMEM((batch * 8, 128), F32),
        pltpu.VMEM((batch * 8, 128), F32),
        pltpu.VMEM((BLK * 8, 128), F32),
        pltpu.VMEM((batch, qcols), BF),
        pltpu.VMEM((nblk, BLK) + k_cache.shape[2:], BF),
        pltpu.VMEM((nblk, BLK) + v_cache.shape[2:], BF),
        pltpu.SemaphoreType.DMA((9,)),
        pltpu.SemaphoreType.DMA((2, nblk)),
        pltpu.SemaphoreType.DMA((2, nblk)),
    ]
    if not has_qkv:
        hidden, norm = source[:2]
        dim = hidden.shape[1]
        scratch += [pltpu.VMEM(hidden.shape, BF), pltpu.VMEM(norm.shape, BF), pltpu.VMEM((dim, cols), BF), pltpu.VMEM(hidden.shape, BF)]
    return pl.pallas_call(
        functools.partial(attn_kernel, layer, has_qkv, prev is not None),
        out_shape=(jax.ShapeDtypeStruct((batch, qcols), BF),
                   jax.ShapeDtypeStruct(k_cache.shape, BF), jax.ShapeDtypeStruct(v_cache.shape, BF)),
        in_specs=[anyspec] * len(args),
        out_specs=(anyspec, anyspec, anyspec),
        scratch_shapes=scratch,
        input_output_aliases=aliases,
        compiler_params=pltpu.CompilerParams(vmem_limit_bytes=62 * 2**20),
        cost_estimate=pl.CostEstimate(flops=2 * batch * 3072 * cols, bytes_accessed=76 * 2**20, transcendentals=0),
        name=f"attn{layer}",
    )(*args)


COPY_HOLD = 9


def write_kernel(layer, pos_hbm, new_hbm, k_hbm, v_hbm, k_prev, v_prev, ko_hbm, vo_hbm, pos_ref, new, k_rows, v_rows, kbuf, vbuf, sem, insem, outsem):
    nblk = kbuf.shape[0]
    batch = nblk * BLK
    first = [pltpu.make_async_copy(pos_hbm, pos_ref, sem.at[0]), pltpu.make_async_copy(new_hbm, new, sem.at[1])]
    for c in first:
        c.start()

    def in_copies(i):
        rows = pl.ds(i * BLK, BLK)
        return (pltpu.make_async_copy(k_hbm.at[layer, rows], kbuf.at[i], insem.at[0, i]),
                pltpu.make_async_copy(v_hbm.at[layer, rows], vbuf.at[i], insem.at[1, i]))

    def out_copies(i):
        rows = pl.ds(i * BLK, BLK)
        return (pltpu.make_async_copy(kbuf.at[i], ko_hbm.at[layer, rows], outsem.at[0, i]),
                pltpu.make_async_copy(vbuf.at[i], vo_hbm.at[layer, rows], outsem.at[1, i]))

    @pl.loop(0, nblk)
    def _(i):
        for c in in_copies(i):
            c.start()

    for c in first:
        c.wait()
    for h in range(2):
        k_vec = new[h].astype(F32)
        v_vec = new[2 + h].astype(F32)
        for r in range(4):
            k_rows[pl.ds(2 * r + h, batch, stride=8), :] = k_vec
            v_rows[pl.ds(2 * r + h, batch, stride=8), :] = v_vec
    seq_in_group = lax.broadcasted_iota(jnp.int32, (16, 128), 0) >> 1

    @pl.loop(0, nblk)
    def _(i):
        for c in in_copies(i):
            c.wait()
        for b in range(BLK):
            pos = pos_ref[i * BLK + b]
            group = pl.ds(pl.multiple_of((pos >> 3) * 16, 16), 16)
            hit = seq_in_group == (pos & 7)
            rows = pl.ds(pl.multiple_of((i * BLK + b) * 8, 8), 8)
            for buf, rows_ref in ((kbuf, k_rows), (vbuf, v_rows)):
                new8 = rows_ref[rows, :]
                new16 = jnp.concatenate([new8, new8], axis=0)
                old16 = buf[i, b, group, :].astype(F32)
                buf[i, b, group, :] = jnp.where(hit, new16, old16).astype(BF)

        @pl.when(i == COPY_HOLD)
        def _():
            @pl.loop(0, COPY_HOLD)
            def _(j):
                for c in out_copies(j):
                    c.start()

        @pl.when(i >= COPY_HOLD)
        def _():
            for c in out_copies(i):
                c.start()

    @pl.loop(0, nblk)
    def _(i):
        for c in out_copies(i):
            c.wait()


def write_rows(layer, positions, new, k_cache, v_cache, prev):
    batch = positions.shape[0]
    nblk = batch // BLK
    anyspec = pl.BlockSpec(memory_space=pl.ANY)
    return pl.pallas_call(
        functools.partial(write_kernel, layer),
        out_shape=(jax.ShapeDtypeStruct(k_cache.shape, BF), jax.ShapeDtypeStruct(v_cache.shape, BF)),
        in_specs=[anyspec] * 6,
        out_specs=(anyspec, anyspec),
        scratch_shapes=[
            pltpu.SMEM((batch,), jnp.int32),
            pltpu.VMEM(new.shape, BF),
            pltpu.VMEM((batch * 8, 128), F32),
            pltpu.VMEM((batch * 8, 128), F32),
            pltpu.VMEM((nblk, BLK) + k_cache.shape[2:], BF),
            pltpu.VMEM((nblk, BLK) + v_cache.shape[2:], BF),
            pltpu.SemaphoreType.DMA((2,)),
            pltpu.SemaphoreType.DMA((2, nblk)),
            pltpu.SemaphoreType.DMA((2, nblk)),
        ],
        input_output_aliases={4: 0, 5: 1},
        compiler_params=pltpu.CompilerParams(vmem_limit_bytes=67043328),
        cost_estimate=pl.CostEstimate(flops=0, bytes_accessed=67 * 2**20, transcendentals=0),
        name="write_rows",
    )(positions, new, k_cache, v_cache, *prev)


CW = 512
HALF = 128
GC = 4
SLOT = 8


def mega_kernel(pos_hbm, table_hbm, att_hbm, x_hbm, mnorm_hbm, anorm_hbm, wo_hbm, wg_hbm, wu_hbm, wd_hbm, wq_hbm, wk_hbm, wv_hbm, k_hbm, v_hbm,
                out_hbm, new_hbm,
                pos_ref, table, cs, wo, wg, wu, wd, wqkv, att, x, mnorm, anorm, h, act, qkv, q_rows, k_rows, v_rows, o_rows, new,
                own, sd, sx, rd, rx,
                wosem, gsem, usem, wsem, isem, sd_sem, sx_sem, sg_sem, rd_sem, rx_sem, ra_sem, osem):
    dim = x.shape[1]
    nch = dim // 2 // CW
    ncol = wg.shape[0]
    qcols = wq_hbm.shape[2]
    kcols = wk_hbm.shape[2]
    heads = qcols // 128
    tp = lax.axis_index("tp")
    core = lax.rem(tp, 2)
    sib = tp + 1 - 2 * core
    peer = lax.rem(tp + 2, 4)
    mine = pl.multiple_of(core * (dim // 2), CW)
    theirs = pl.multiple_of((1 - core) * (dim // 2), CW)

    def chunk(side, k):
        return pl.ds(pl.multiple_of((theirs, mine)[side] + k * CW, CW), CW)

    def wo_copy(layer, side, k):
        return pltpu.make_async_copy(wo_hbm.at[layer, :, chunk(side, k)], wo.at[:, chunk(side, k)], wosem.at[side, k])

    def gu_copies(layer, c):
        cols = pl.ds(pl.multiple_of(c * 128, 128), 128)
        return (pltpu.make_async_copy(wg_hbm.at[layer, :, cols], wg.at[c], gsem.at[c]),
                pltpu.make_async_copy(wu_hbm.at[layer, :, cols], wu.at[c], usem.at[c]))

    def kv_copies(half, c):
        src = pl.ds(pl.multiple_of((half * HALF + c * SLOT) * 256, 2048), SLOT * 256)
        dst = pl.ds(0, SLOT * 256)
        return (pltpu.make_async_copy(k_hbm.at[1, src], wg.at[c, dst], gsem.at[c]),
                pltpu.make_async_copy(v_hbm.at[1, src], wu.at[c, dst], usem.at[c]))

    def wd_copy(layer):
        return pltpu.make_async_copy(wd_hbm.at[layer], wd, wsem.at[0])

    att_copy = pltpu.make_async_copy(att_hbm, att, isem.at[0])
    x_copy = pltpu.make_async_copy(x_hbm, x, isem.at[1])
    small = [pltpu.make_async_copy(mnorm_hbm, mnorm, isem.at[2]), pltpu.make_async_copy(anorm_hbm, anorm, isem.at[3]),
             pltpu.make_async_copy(pos_hbm, pos_ref, isem.at[4]), pltpu.make_async_copy(table_hbm, table, isem.at[5])]
    qkv_loads = [
        pltpu.make_async_copy(wq_hbm.at[1], wqkv.at[:, pl.ds(0, qcols)], wsem.at[1]),
        pltpu.make_async_copy(wk_hbm.at[1], wqkv.at[:, pl.ds(qcols, kcols)], wsem.at[2]),
        pltpu.make_async_copy(wv_hbm.at[1], wqkv.at[:, pl.ds(qcols + kcols, kcols)], wsem.at[3]),
    ]
    att_copy.start()
    wo_copy(0, 0, 0).start()
    wo_copy(0, 1, 0).start()
    x_copy.start()
    for k in range(1, nch):
        wo_copy(0, 0, k).start()
        wo_copy(0, 1, k).start()
    for c in small:
        c.start()

    barrier = pltpu.get_barrier_semaphore()
    for other in (sib, peer):
        pl.semaphore_signal(barrier, inc=1, device_id={"tp": other}, device_id_type=MESH)
    pl.semaphore_wait(barrier, 2)

    def to_sib(ph, k):
        return pltpu.make_async_remote_copy(sd.at[ph % 2, k], rd.at[ph % 4, k], sd_sem.at[ph, k], rd_sem.at[ph, k],
                                            device_id={"tp": sib}, device_id_type=MESH)

    def to_peer(ph, k):
        return pltpu.make_async_remote_copy(sx.at[ph % 2, k], rx.at[ph % 4, k], sx_sem.at[ph, k], rx_sem.at[ph, k],
                                            device_id={"tp": peer}, device_id_type=MESH)

    def final(ph):
        return ph >= 6

    def share(ph, k):
        rows = pl.ds((ph % 2) * HALF, HALF)
        dst = out_hbm if final(ph) else x
        return pltpu.make_async_remote_copy(x.at[rows, chunk(1, k)], dst.at[rows, chunk(1, k)], sg_sem.at[ph, k], ra_sem.at[ph, k],
                                            device_id={"tp": sib}, device_id_type=MESH)

    def keep(ph, k):
        rows = pl.ds((ph % 2) * HALF, HALF)
        return pltpu.make_async_copy(x.at[rows, chunk(1, k)], out_hbm.at[rows, chunk(1, k)], osem.at[ph % 2, k])

    def reduce_start(ph, lhs, w_ref, load):
        def dot(side, k):
            if load is not None:
                load(side, k).wait()
            return jnp.dot(lhs, w_ref[:, chunk(side, k)], preferred_element_type=F32)

        def forward(k):
            to_sib(ph, k).wait_recv()
            sx[ph % 2, k] = (own[k] + rd[ph % 4, k].astype(F32)).astype(BF)
            to_peer(ph, k).start()

        for k in range(nch):
            sd[ph % 2, k] = dot(0, k).astype(BF)
            to_sib(ph, k).start()
            if k > 0:
                forward(k - 1)
            own[k] = dot(1, k)
        forward(nch - 1)
        for k in range(nch):
            to_sib(ph, k).wait_send()

    def reduce_end(ph):
        rows = pl.ds((ph % 2) * HALF, HALF)
        for k in range(nch):
            to_peer(ph, k).wait()
            total = (sx[ph % 2, k].astype(F32) + rx[ph % 4, k].astype(F32)).astype(BF)
            x[rows, chunk(1, k)] = (x[rows, chunk(1, k)].astype(F32) + total.astype(F32)).astype(BF)
            share(ph, k).start()
            if final(ph):
                keep(ph, k).start()
        for k in range(nch):
            share(ph, k).wait()

    def gate_up(layer, half):
        rows = pl.ds(half * HALF, HALF)
        h[...] = normed(x[rows, :].astype(F32), mnorm[layer:layer + 1, :].astype(F32))

        @pl.loop(0, ncol // GC)
        def _(n):
            if half == 0:
                for c in range(GC):
                    for cp in gu_copies(layer, n * GC + c):
                        cp.wait()
            wide = lambda ref: jnp.concatenate([ref[n * GC + c] for c in range(GC)], axis=1)
            g = jnp.dot(h[...], wide(wg), preferred_element_type=F32).astype(BF).astype(F32)
            u = jnp.dot(h[...], wide(wu), preferred_element_type=F32).astype(BF).astype(F32)
            cols = pl.ds(pl.multiple_of(n * GC * 128, GC * 128), GC * 128)
            act[:, cols] = (g * jax.nn.sigmoid(g) * u).astype(BF)

    def qkv_rope(half):
        rows = pl.ds(half * HALF, HALF)
        h[...] = normed(x[rows, :].astype(F32), anorm[1:2, :].astype(F32))

        @pl.loop(0, qkv.shape[0])
        def _(n):
            cols = pl.ds(pl.multiple_of(n * 256, 256), 256)
            qkv[n] = jnp.dot(h[...], wqkv[:, cols], preferred_element_type=F32).astype(BF)

        cos_b = cs[rows, 0:128]
        sin_b = cs[rows, 128:256]

        def piece(n, i):
            return qkv[n, :, i * 128:i * 128 + 128].astype(F32)

        def rope(vec):
            return (vec * cos_b + pltpu.roll(vec, 64, 1) * sin_b).astype(BF)

        k_new = [rope(piece(heads // 2, i)) for i in range(2)]
        v_new = [piece(heads // 2 + 1, i) for i in range(2)]
        for i in range(2):
            new[i, rows, :] = k_new[i]
            new[2 + i, rows, :] = v_new[i].astype(BF)
        zero = jnp.zeros((HALF, 128), F32)
        for j in range(8):
            out_rows = pl.ds(j, HALF, stride=8)
            kv = 0 if j < heads // 2 else 1
            q_rows[out_rows, :] = rope(piece(j // 2, j % 2)).astype(F32) if j < heads else zero
            k_rows[out_rows, :] = k_new[kv].astype(F32)
            v_rows[out_rows, :] = v_new[kv]

    col = lax.broadcasted_iota(jnp.int32, (8, 256), 1)
    row = lax.broadcasted_iota(jnp.int32, (8, 256), 0)
    key_row = jnp.where((col & 1) == jnp.where(row >= heads // 2, 1, 0), col >> 1, 4096)
    scale = 128 ** -0.5

    def attend(half):
        @pl.loop(0, ncol // 2)
        def _(i):
            for c in range(2):
                for cp in kv_copies(half, 2 * i + c):
                    cp.wait()
            pairs = range(SLOT)
            zero8 = jnp.zeros((8, 128), F32)

            def rows8(p, b):
                return pl.ds(pl.multiple_of((i * 2 * SLOT + 2 * p + b) * 8, 8), 8)

            def pos(p, b):
                return pos_ref[half * HALF + i * 2 * SLOT + 2 * p + b]

            def both(ref, p):
                r = 2 * p % SLOT
                slot = 2 * i + 2 * p // SLOT
                return jnp.concatenate([ref[slot, r * 256:(r + 1) * 256, :], ref[slot, (r + 1) * 256:(r + 2) * 256, :]], axis=1)

            scores, fresh = [], []
            for p in pairs:
                qa = q_rows[rows8(p, 0), :]
                qb = q_rows[rows8(p, 1), :]
                q2 = jnp.concatenate([jnp.concatenate([qa, zero8], axis=1), jnp.concatenate([zero8, qb], axis=1)], axis=0).astype(BF)
                scores.append(lax.dot_general(q2, both(wg, p), (((1,), (1,)), ((), ())), preferred_element_type=F32))
                prod = jnp.concatenate([qa * k_rows[rows8(p, 0), :], qb * k_rows[rows8(p, 1), :]], axis=0)
                fresh.append(jnp.sum(prod, axis=-1, keepdims=True) * scale)
            weights, last = [], []
            for p in pairs:
                before = jnp.concatenate([key_row < pos(p, 0), key_row < pos(p, 1)], axis=0)
                s = jnp.where(before, scores[p] * scale, NEG)
                peak = jnp.maximum(jnp.max(s, axis=-1, keepdims=True), fresh[p])
                e = jnp.exp(s - peak)
                e_new = jnp.exp(fresh[p] - peak)
                inv = 1.0 / (jnp.sum(e, axis=-1, keepdims=True) + e_new)
                weights.append((e * inv).astype(BF))
                last.append((e_new * inv).astype(BF).astype(F32))
            outs = [jnp.dot(weights[p], both(wu, p), preferred_element_type=F32) for p in pairs]
            for p in pairs:
                o_rows[rows8(p, 0), :] = outs[p][0:8, 0:128] + last[p][0:8] * v_rows[rows8(p, 0), :]
                o_rows[rows8(p, 1), :] = outs[p][8:16, 128:256] + last[p][8:16] * v_rows[rows8(p, 1), :]
            for c in range(2):
                for cp in (kv_copies(1, 2 * i + c) if half == 0 else gu_copies(1, 2 * i + c)):
                    cp.start()

        rows = pl.ds(half * HALF, HALF)
        for j in range(heads):
            att[rows, j * 128:(j + 1) * 128] = o_rows[pl.ds(j, HALF, stride=8), :].astype(BF)

    def att_half(half):
        return att[half * HALF:(half + 1) * HALF, :]

    att_copy.wait()
    x_copy.wait()
    reduce_start(0, att_half(0), wo, lambda side, k: wo_copy(0, side, k))

    @pl.loop(0, ncol)
    def _(c):
        for cp in gu_copies(0, c):
            cp.start()

    wd_copy(0).start()
    for c in qkv_loads:
        c.start()
    reduce_start(1, att_half(1), wo, None)
    for k in range(nch):
        wo_copy(1, 0, k).start()
        wo_copy(1, 1, k).start()
    for c in small:
        c.wait()

    @pl.loop(0, 2 * HALF // 8)
    def _(i):
        for b in range(8):
            r = i * 8 + b
            cs[pl.ds(r, 1), :] = table[pl.ds(pos_ref[r], 1), :]

    for half in range(2):
        reduce_end(half)
        gate_up(0, half)
        if half == 0:
            wd_copy(0).wait()
        else:
            @pl.loop(0, ncol)
            def _(c):
                for cp in kv_copies(0, c):
                    cp.start()

        reduce_start(2 + half, act[...], wd, None)
    wd_copy(1).start()
    for c in qkv_loads:
        c.wait()
    for half in range(2):
        reduce_end(2 + half)
        qkv_rope(half)
        attend(half)
        reduce_start(4 + half, att_half(half), wo, (lambda side, k: wo_copy(1, side, k)) if half == 0 else None)
    new_copy = pltpu.make_async_copy(new, new_hbm, isem.at[6])
    new_copy.start()
    for half in range(2):
        reduce_end(4 + half)
        gate_up(1, half)
        if half == 0:
            wd_copy(1).wait()
        reduce_start(6 + half, act[...], wd, None)
    for half in range(2):
        reduce_end(6 + half)
    new_copy.wait()
    for half in range(2):
        for k in range(nch):
            keep(6 + half, k).wait()


def mega(positions, table, att, hidden, mnorm, anorm, wo, wg, wu, wd, wq, wk, wv, k_rows, v_rows):
    batch, dim = hidden.shape
    nch = dim // 2 // CW
    cols = wq.shape[2] + 2 * wk.shape[2]
    ncol = wg.shape[2] // 128
    anyspec = pl.BlockSpec(memory_space=pl.ANY)
    msg = lambda n: pltpu.VMEM((n, nch, HALF, CW), BF)
    sems = pltpu.SemaphoreType.DMA((8, nch))
    rows = pltpu.VMEM((HALF * 8, 128), F32)
    args = [positions, table, att, hidden, mnorm, anorm, wo, wg, wu, wd, wq, wk, wv, k_rows, v_rows]
    return pl.pallas_call(
        mega_kernel,
        out_shape=(jax.ShapeDtypeStruct((batch, dim), BF), jax.ShapeDtypeStruct((4, batch, 128), BF)),
        in_specs=[anyspec] * len(args),
        out_specs=(anyspec, anyspec),
        scratch_shapes=[
            pltpu.SMEM((batch,), jnp.int32), pltpu.VMEM(table.shape, F32), pltpu.VMEM((batch, table.shape[1]), F32),
            pltpu.VMEM(wo.shape[1:], BF), pltpu.VMEM((ncol, dim, 128), BF), pltpu.VMEM((ncol, dim, 128), BF), pltpu.VMEM(wd.shape[1:], BF),
            pltpu.VMEM((dim, cols), BF), pltpu.VMEM(att.shape, BF), pltpu.VMEM(hidden.shape, BF),
            pltpu.VMEM(mnorm.shape, BF), pltpu.VMEM(anorm.shape, BF),
            pltpu.VMEM((HALF, dim), BF), pltpu.VMEM((HALF, wd.shape[1]), BF), pltpu.VMEM((cols // 256, HALF, 256), BF),
            rows, rows, rows, rows, pltpu.VMEM((4, batch, 128), BF),
            pltpu.VMEM((nch, HALF, CW), F32), msg(2), msg(2), msg(4), msg(4),
            pltpu.SemaphoreType.DMA((2, nch)), pltpu.SemaphoreType.DMA((ncol,)), pltpu.SemaphoreType.DMA((ncol,)),
            pltpu.SemaphoreType.DMA((4,)), pltpu.SemaphoreType.DMA((7,)),
            sems, sems, sems, sems, sems, sems, pltpu.SemaphoreType.DMA((2, nch)),
        ],
        compiler_params=pltpu.CompilerParams(collective_id=0, has_side_effects=True, vmem_limit_bytes=67043328),
        name="mega",
    )(*args)


def solution(mesh):
    row_spec = P('dp', None)
    pos_spec = P('dp')
    cache_spec = P(None, 'dp', None, 'tp', None)
    norm_spec = P(None, None)
    col_spec = P(None, None, 'tp')
    split_rows = P(None, 'tp', None)

    def local_step(hidden, positions, k_cache, v_cache, attn_norm, w_query, w_key, w_value, w_out, mlp_norm, w_gate, w_up, w_down):
        cache_shape = k_cache.shape
        flat = (cache_shape[0], cache_shape[1], cache_shape[2] * cache_shape[3], cache_shape[4])
        k_flat, v_flat = k_cache.reshape(flat), v_cache.reshape(flat)
        table = jnp.asarray(rope_table(cache_shape[2], cache_shape[4]))
        source = (hidden, attn_norm, w_query, w_key, w_value)
        att, *caches = attention(0, positions, table, source, k_flat, v_flat, None, w_query.shape[2], w_key.shape[2])
        rows = (cache_shape[0], -1, cache_shape[4])
        hidden, new = mega(positions, table, att, hidden, mlp_norm, attn_norm, w_out, w_gate, w_up, w_down, w_query, w_key, w_value,
                           k_cache.reshape(rows), v_cache.reshape(rows))
        caches = write_rows(1, positions, new, k_flat, v_flat, caches)
        return hidden, caches[0].reshape(cache_shape), caches[1].reshape(cache_shape)

    return jax.shard_map(local_step, mesh=mesh, in_specs=(row_spec, pos_spec, cache_spec, cache_spec, norm_spec, col_spec, col_spec, col_spec, split_rows, norm_spec, col_spec, col_spec, split_rows), out_specs=(row_spec, cache_spec, cache_spec), check_vma=False)
```

```python
import functools
import math
import jax
import jax.numpy as jnp
import numpy as np
from jax import lax
from jax.experimental import pallas as pl
from jax.experimental.pallas import tpu as pltpu
from jax.sharding import PartitionSpec as P

BF = jnp.bfloat16
F32 = jnp.float32
MESH = pl.DeviceIdType.MESH
EPS = 1e-5
NEG = -1e30


def rope_table(rows, head_dim):
    half_dim = head_dim // 2
    inv_freq = np.power(np.float32(500000.0), -np.arange(half_dim, dtype=np.float32) * np.float32(2.0 / head_dim)).astype(np.float32)
    wavelen = (np.float32(2.0 * math.pi) / inv_freq).astype(np.float32)
    smooth = (np.float32(8192.0) / wavelen - np.float32(1.0)) / np.float32(3.0)
    blended = (np.float32(1.0) - smooth) * inv_freq / np.float32(8.0) + smooth * inv_freq
    scaled = np.where(wavelen < 2048.0, inv_freq, np.where(wavelen > 8192.0, inv_freq / np.float32(8.0), blended)).astype(np.float32)
    angles = np.arange(rows, dtype=np.float32)[:, None] * scaled[None, :]
    cos, sin = np.cos(angles.astype(np.float64)), np.sin(angles.astype(np.float64))
    return np.concatenate([cos, cos, -sin, sin], axis=-1).astype(np.float32)


def normed(x_f32, weight_f32):
    mean_sq = jnp.mean(x_f32 * x_f32, axis=-1, keepdims=True)
    return (x_f32 * lax.rsqrt(mean_sq + EPS) * weight_f32).astype(BF)


BLK = 16
HOLD = 4


def attn_kernel(layer, has_qkv, aliased, *refs):
    pos_hbm, table_hbm = refs[:2]
    if has_qkv:
        qkv_hbm, k_hbm, v_hbm = refs[2:5]
        refs = refs[5:]
    else:
        x_hbm, norm_hbm, wq_hbm, wk_hbm, wv_hbm, k_hbm, v_hbm = refs[2:9]
        refs = refs[9:]
    if aliased:
        refs = refs[2:]
    att_hbm, ko_hbm, vo_hbm, pos_ref, table, qkv, cs, q_rows, k_rows, v_rows, o_rows, att, kbuf, vbuf, sem, insem, outsem, *rest = refs
    nblk = kbuf.shape[0]
    batch = nblk * BLK
    heads = att.shape[1] // 128

    pos_copy = pltpu.make_async_copy(pos_hbm, pos_ref, sem.at[0])
    table_copy = pltpu.make_async_copy(table_hbm, table, sem.at[1])
    pos_copy.start()
    table_copy.start()
    if has_qkv:
        first = [pltpu.make_async_copy(qkv_hbm, qkv, sem.at[2])]
    else:
        x_buf, norm, w_buf, h_buf = rest
        qcols = wq_hbm.shape[2]
        kcols = wk_hbm.shape[2]
        x_copies = [pltpu.make_async_copy(x_hbm, x_buf, sem.at[3]), pltpu.make_async_copy(norm_hbm, norm, sem.at[4])]
        for c in x_copies:
            c.start()
        first = [
            pltpu.make_async_copy(wq_hbm.at[layer], w_buf.at[:, pl.ds(0, qcols)], sem.at[5]),
            pltpu.make_async_copy(wk_hbm.at[layer], w_buf.at[:, pl.ds(qcols, kcols)], sem.at[6]),
            pltpu.make_async_copy(wv_hbm.at[layer], w_buf.at[:, pl.ds(qcols + kcols, kcols)], sem.at[7]),
        ]
    for c in first:
        c.start()

    def in_copies(i):
        rows = pl.ds(i * BLK, BLK)
        return (pltpu.make_async_copy(k_hbm.at[layer, rows], kbuf.at[i], insem.at[0, i]),
                pltpu.make_async_copy(v_hbm.at[layer, rows], vbuf.at[i], insem.at[1, i]))

    def out_copies(i):
        rows = pl.ds(i * BLK, BLK)
        return (pltpu.make_async_copy(kbuf.at[i], ko_hbm.at[layer, rows], outsem.at[0, i]),
                pltpu.make_async_copy(vbuf.at[i], vo_hbm.at[layer, rows], outsem.at[1, i]))

    @pl.loop(0, nblk)
    def _(i):
        for c in in_copies(i):
            c.start()

    pos_copy.wait()
    table_copy.wait()

    @pl.loop(0, batch // 8)
    def _(i):
        for b in range(8):
            r = i * 8 + b
            cs[pl.ds(r, 1), :] = table[pl.ds(pos_ref[r], 1), :]

    if not has_qkv:
        for c in x_copies:
            c.wait()
        h_buf[...] = normed(x_buf[...].astype(F32), norm[layer:layer + 1, :].astype(F32))
    for c in first:
        c.wait()
    if not has_qkv:
        @pl.loop(0, (qcols + 2 * kcols) // 256)
        def _(n):
            cols = pl.ds(pl.multiple_of(n * 256, 256), 256)
            qkv[n] = jnp.dot(h_buf[...], w_buf[:, cols], preferred_element_type=F32).astype(BF)

    cos_b = cs[:, 0:128]
    sin_b = cs[:, 128:256]

    def piece(n, h):
        return qkv[n, :, h * 128:h * 128 + 128].astype(F32)

    def rope(vec):
        return (vec * cos_b + pltpu.roll(vec, 64, 1) * sin_b).astype(BF).astype(F32)

    zero = jnp.zeros((batch, 128), F32)
    for j in range(8):
        q_rows[pl.ds(j, batch, stride=8), :] = rope(piece(j // 2, j % 2)) if j < heads else zero
    for h in range(2):
        k_vec = rope(piece(heads // 2, h))
        v_vec = piece(heads // 2 + 1, h)
        for r in range(4):
            k_rows[pl.ds(2 * r + h, batch, stride=8), :] = k_vec
            v_rows[pl.ds(2 * r + h, batch, stride=8), :] = v_vec

    col = lax.broadcasted_iota(jnp.int32, (8, 256), 1)
    row = lax.broadcasted_iota(jnp.int32, (8, 256), 0)
    own = (col & 1) == jnp.where(row >= heads // 2, 1, 0)
    key_row = jnp.where(own, col >> 1, 4096)
    seq_in_group = lax.broadcasted_iota(jnp.int32, (16, 128), 0) >> 1
    scale = 128 ** -0.5

    @pl.loop(0, nblk)
    def _(i):
        for c in in_copies(i):
            c.wait()
        for b in range(BLK):
            pos = pos_ref[i * BLK + b]
            group = pl.ds(pl.multiple_of((pos >> 3) * 16, 16), 16)
            hit = seq_in_group == (pos & 7)
            rows = pl.ds(pl.multiple_of((i * BLK + b) * 8, 8), 8)
            for buf, new in ((kbuf, k_rows), (vbuf, v_rows)):
                new8 = new[rows, :]
                new16 = jnp.concatenate([new8, new8], axis=0)
                old16 = buf[i, b, group, :].astype(F32)
                buf[i, b, group, :] = jnp.where(hit, new16, old16).astype(BF)
        zero8 = jnp.zeros((8, 128), F32)
        pairs = range(BLK // 2)
        scores = []
        for p in pairs:
            first = i * BLK + 2 * p
            qa = q_rows[pl.ds(pl.multiple_of(first * 8, 8), 8), :]
            qb = q_rows[pl.ds(pl.multiple_of(first * 8 + 8, 8), 8), :]
            q2 = jnp.concatenate([jnp.concatenate([qa, zero8], axis=1), jnp.concatenate([zero8, qb], axis=1)], axis=0).astype(BF)
            k2 = jnp.concatenate([kbuf[i, 2 * p], kbuf[i, 2 * p + 1]], axis=1)
            scores.append(lax.dot_general(q2, k2, (((1,), (1,)), ((), ())), preferred_element_type=F32))
        weights = []
        for p in pairs:
            first = i * BLK + 2 * p
            keep = jnp.concatenate([key_row <= pos_ref[first], key_row <= pos_ref[first + 1]], axis=0)
            s = jnp.where(keep, scores[p] * scale, NEG)
            e = jnp.exp(s - jnp.max(s, axis=-1, keepdims=True))
            weights.append((e * (1.0 / jnp.sum(e, axis=-1, keepdims=True))).astype(BF))
        outs = []
        for p in pairs:
            v2 = jnp.concatenate([vbuf[i, 2 * p], vbuf[i, 2 * p + 1]], axis=1)
            outs.append(jnp.dot(weights[p], v2, preferred_element_type=F32))

        @pl.when(i == HOLD)
        def _():
            @pl.loop(0, HOLD)
            def _(j):
                for c in out_copies(j):
                    c.start()

        @pl.when(i >= HOLD)
        def _():
            for c in out_copies(i):
                c.start()

        for p in pairs:
            o_rows[16 * p:16 * p + 8, :] = outs[p][0:8, 0:128]
            o_rows[16 * p + 8:16 * p + 16, :] = outs[p][8:16, 128:256]
        rows = pl.ds(pl.multiple_of(i * BLK, BLK), BLK)
        for j in range(heads):
            att[rows, j * 128:(j + 1) * 128] = o_rows[pl.ds(j, BLK, stride=8), :].astype(BF)

    att_copy = pltpu.make_async_copy(att, att_hbm, sem.at[8])
    att_copy.start()
    att_copy.wait()

    @pl.loop(0, nblk)
    def _(i):
        for c in out_copies(i):
            c.wait()


def attention(layer, positions, table, source, k_cache, v_cache, prev, qcols, kcols):
    batch = positions.shape[0]
    has_qkv = len(source) == 1
    anyspec = pl.BlockSpec(memory_space=pl.ANY)
    args = [positions, table, *source, k_cache, v_cache]
    aliases = {}
    if prev is not None:
        aliases = {len(args): 1, len(args) + 1: 2}
        args += list(prev)
    cols = qcols + 2 * kcols
    nblk = batch // BLK
    scratch = [
        pltpu.SMEM((batch,), jnp.int32),
        pltpu.VMEM(table.shape, F32),
        pltpu.VMEM((cols // 256, batch, 256), BF),
        pltpu.VMEM((batch, table.shape[1]), F32),
        pltpu.VMEM((batch * 8, 128), F32),
        pltpu.VMEM((batch * 8, 128), F32),
        pltpu.VMEM((batch * 8, 128), F32),
        pltpu.VMEM((BLK * 8, 128), F32),
        pltpu.VMEM((batch, qcols), BF),
        pltpu.VMEM((nblk, BLK) + k_cache.shape[2:], BF),
        pltpu.VMEM((nblk, BLK) + v_cache.shape[2:], BF),
        pltpu.SemaphoreType.DMA((9,)),
        pltpu.SemaphoreType.DMA((2, nblk)),
        pltpu.SemaphoreType.DMA((2, nblk)),
    ]
    if not has_qkv:
        hidden, norm = source[:2]
        dim = hidden.shape[1]
        scratch += [pltpu.VMEM(hidden.shape, BF), pltpu.VMEM(norm.shape, BF), pltpu.VMEM((dim, cols), BF), pltpu.VMEM(hidden.shape, BF)]
    return pl.pallas_call(
        functools.partial(attn_kernel, layer, has_qkv, prev is not None),
        out_shape=(jax.ShapeDtypeStruct((batch, qcols), BF),
                   jax.ShapeDtypeStruct(k_cache.shape, BF), jax.ShapeDtypeStruct(v_cache.shape, BF)),
        in_specs=[anyspec] * len(args),
        out_specs=(anyspec, anyspec, anyspec),
        scratch_shapes=scratch,
        input_output_aliases=aliases,
        compiler_params=pltpu.CompilerParams(vmem_limit_bytes=62 * 2**20),
        cost_estimate=pl.CostEstimate(flops=2 * batch * 3072 * cols, bytes_accessed=76 * 2**20, transcendentals=0),
        name=f"attn{layer}",
    )(*args)


COPY_HOLD = 9


def write_kernel(layer, pos_hbm, new_hbm, k_hbm, v_hbm, k_prev, v_prev, ko_hbm, vo_hbm, pos_ref, new, k_rows, v_rows, kbuf, vbuf, sem, insem, outsem):
    nblk = kbuf.shape[0]
    batch = nblk * BLK
    first = [pltpu.make_async_copy(pos_hbm, pos_ref, sem.at[0]), pltpu.make_async_copy(new_hbm, new, sem.at[1])]
    for c in first:
        c.start()

    def in_copies(i):
        rows = pl.ds(i * BLK, BLK)
        return (pltpu.make_async_copy(k_hbm.at[layer, rows], kbuf.at[i], insem.at[0, i]),
                pltpu.make_async_copy(v_hbm.at[layer, rows], vbuf.at[i], insem.at[1, i]))

    def out_copies(i):
        rows = pl.ds(i * BLK, BLK)
        return (pltpu.make_async_copy(kbuf.at[i], ko_hbm.at[layer, rows], outsem.at[0, i]),
                pltpu.make_async_copy(vbuf.at[i], vo_hbm.at[layer, rows], outsem.at[1, i]))

    @pl.loop(0, nblk)
    def _(i):
        for c in in_copies(i):
            c.start()

    for c in first:
        c.wait()
    for h in range(2):
        k_vec = new[h].astype(F32)
        v_vec = new[2 + h].astype(F32)
        for r in range(4):
            k_rows[pl.ds(2 * r + h, batch, stride=8), :] = k_vec
            v_rows[pl.ds(2 * r + h, batch, stride=8), :] = v_vec
    seq_in_group = lax.broadcasted_iota(jnp.int32, (16, 128), 0) >> 1

    @pl.loop(0, nblk)
    def _(i):
        for c in in_copies(i):
            c.wait()
        for b in range(BLK):
            pos = pos_ref[i * BLK + b]
            group = pl.ds(pl.multiple_of((pos >> 3) * 16, 16), 16)
            hit = seq_in_group == (pos & 7)
            rows = pl.ds(pl.multiple_of((i * BLK + b) * 8, 8), 8)
            for buf, rows_ref in ((kbuf, k_rows), (vbuf, v_rows)):
                new8 = rows_ref[rows, :]
                new16 = jnp.concatenate([new8, new8], axis=0)
                old16 = buf[i, b, group, :].astype(F32)
                buf[i, b, group, :] = jnp.where(hit, new16, old16).astype(BF)

        @pl.when(i == COPY_HOLD)
        def _():
            @pl.loop(0, COPY_HOLD)
            def _(j):
                for c in out_copies(j):
                    c.start()

        @pl.when(i >= COPY_HOLD)
        def _():
            for c in out_copies(i):
                c.start()

    @pl.loop(0, nblk)
    def _(i):
        for c in out_copies(i):
            c.wait()


def write_rows(layer, positions, new, k_cache, v_cache, prev):
    batch = positions.shape[0]
    nblk = batch // BLK
    anyspec = pl.BlockSpec(memory_space=pl.ANY)
    return pl.pallas_call(
        functools.partial(write_kernel, layer),
        out_shape=(jax.ShapeDtypeStruct(k_cache.shape, BF), jax.ShapeDtypeStruct(v_cache.shape, BF)),
        in_specs=[anyspec] * 6,
        out_specs=(anyspec, anyspec),
        scratch_shapes=[
            pltpu.SMEM((batch,), jnp.int32),
            pltpu.VMEM(new.shape, BF),
            pltpu.VMEM((batch * 8, 128), F32),
            pltpu.VMEM((batch * 8, 128), F32),
            pltpu.VMEM((nblk, BLK) + k_cache.shape[2:], BF),
            pltpu.VMEM((nblk, BLK) + v_cache.shape[2:], BF),
            pltpu.SemaphoreType.DMA((2,)),
            pltpu.SemaphoreType.DMA((2, nblk)),
            pltpu.SemaphoreType.DMA((2, nblk)),
        ],
        input_output_aliases={4: 0, 5: 1},
        compiler_params=pltpu.CompilerParams(vmem_limit_bytes=67043328),
        cost_estimate=pl.CostEstimate(flops=0, bytes_accessed=67 * 2**20, transcendentals=0),
        name="write_rows",
    )(positions, new, k_cache, v_cache, *prev)


CW = 512
HALF = 128
GC = 4
SLOT = 8


def mega_kernel(pos_hbm, table_hbm, att_hbm, x_hbm, mnorm_hbm, anorm_hbm, wo_hbm, wg_hbm, wu_hbm, wd_hbm, wq_hbm, wk_hbm, wv_hbm, k_hbm, v_hbm,
                out_hbm, new_hbm,
                pos_ref, table, cs, wo, wg, wu, wd, wqkv, att, x, mnorm, anorm, h, act, qkv, q_rows, k_rows, v_rows, o_rows, s_buf, new,
                own, sd, sx, rd, rx,
                wosem, gsem, usem, wsem, isem, sd_sem, sx_sem, sg_sem, rd_sem, rx_sem, ra_sem, osem):
    dim = x.shape[1]
    nch = dim // 2 // CW
    ncol = wg.shape[0]
    qcols = wq_hbm.shape[2]
    kcols = wk_hbm.shape[2]
    heads = qcols // 128
    tp = lax.axis_index("tp")
    core = lax.rem(tp, 2)
    sib = tp + 1 - 2 * core
    peer = lax.rem(tp + 2, 4)
    mine = pl.multiple_of(core * (dim // 2), CW)
    theirs = pl.multiple_of((1 - core) * (dim // 2), CW)

    def chunk(side, k):
        return pl.ds(pl.multiple_of((theirs, mine)[side] + k * CW, CW), CW)

    def wo_copy(layer, side, k):
        return pltpu.make_async_copy(wo_hbm.at[layer, :, chunk(side, k)], wo.at[:, chunk(side, k)], wosem.at[side, k])

    def gu_copies(layer, c):
        cols = pl.ds(pl.multiple_of(c * 128, 128), 128)
        return (pltpu.make_async_copy(wg_hbm.at[layer, :, cols], wg.at[c], gsem.at[c]),
                pltpu.make_async_copy(wu_hbm.at[layer, :, cols], wu.at[c], usem.at[c]))

    def kv_copies(half, c):
        src = pl.ds(pl.multiple_of((half * HALF + c * SLOT) * 256, 2048), SLOT * 256)
        dst = pl.ds(0, SLOT * 256)
        return (pltpu.make_async_copy(k_hbm.at[1, src], wg.at[c, dst], gsem.at[c]),
                pltpu.make_async_copy(v_hbm.at[1, src], wu.at[c, dst], usem.at[c]))

    def wd_copy(layer):
        return pltpu.make_async_copy(wd_hbm.at[layer], wd, wsem.at[0])

    att_copy = pltpu.make_async_copy(att_hbm, att, isem.at[0])
    x_copy = pltpu.make_async_copy(x_hbm, x, isem.at[1])
    small = [pltpu.make_async_copy(mnorm_hbm, mnorm, isem.at[2]), pltpu.make_async_copy(anorm_hbm, anorm, isem.at[3]),
             pltpu.make_async_copy(pos_hbm, pos_ref, isem.at[4]), pltpu.make_async_copy(table_hbm, table, isem.at[5])]
    qkv_loads = [
        pltpu.make_async_copy(wq_hbm.at[1], wqkv.at[:, pl.ds(0, qcols)], wsem.at[1]),
        pltpu.make_async_copy(wk_hbm.at[1], wqkv.at[:, pl.ds(qcols, kcols)], wsem.at[2]),
        pltpu.make_async_copy(wv_hbm.at[1], wqkv.at[:, pl.ds(qcols + kcols, kcols)], wsem.at[3]),
    ]
    att_copy.start()
    wo_copy(0, 0, 0).start()
    wo_copy(0, 1, 0).start()
    x_copy.start()
    for k in range(1, nch):
        wo_copy(0, 0, k).start()
        wo_copy(0, 1, k).start()
    for c in small:
        c.start()

    barrier = pltpu.get_barrier_semaphore()
    for other in (sib, peer):
        pl.semaphore_signal(barrier, inc=1, device_id={"tp": other}, device_id_type=MESH)
    pl.semaphore_wait(barrier, 2)

    def to_sib(ph, k):
        return pltpu.make_async_remote_copy(sd.at[ph % 2, k], rd.at[ph % 4, k], sd_sem.at[ph, k], rd_sem.at[ph, k],
                                            device_id={"tp": sib}, device_id_type=MESH)

    def to_peer(ph, k):
        return pltpu.make_async_remote_copy(sx.at[ph % 2, k], rx.at[ph % 4, k], sx_sem.at[ph, k], rx_sem.at[ph, k],
                                            device_id={"tp": peer}, device_id_type=MESH)

    def final(ph):
        return ph >= 6

    def share(ph, k):
        rows = pl.ds((ph % 2) * HALF, HALF)
        dst = out_hbm if final(ph) else x
        return pltpu.make_async_remote_copy(x.at[rows, chunk(1, k)], dst.at[rows, chunk(1, k)], sg_sem.at[ph, k], ra_sem.at[ph, k],
                                            device_id={"tp": sib}, device_id_type=MESH)

    def keep(ph, k):
        rows = pl.ds((ph % 2) * HALF, HALF)
        return pltpu.make_async_copy(x.at[rows, chunk(1, k)], out_hbm.at[rows, chunk(1, k)], osem.at[ph % 2, k])

    def reduce_start(ph, lhs, w_ref, load):
        def dot(side, k):
            if load is not None:
                load(side, k).wait()
            return jnp.dot(lhs(), w_ref[:, chunk(side, k)], preferred_element_type=F32)

        def send(k):
            sd[ph % 2, k] = dot(0, k).astype(BF)
            to_sib(ph, k).start()

        def hold(k):
            own[k] = dot(1, k)

        def forward(k):
            to_sib(ph, k).wait_recv()
            sx[ph % 2, k] = (own[k] + rd[ph % 4, k].astype(F32)).astype(BF)
            to_peer(ph, k).start()

        send(0)
        send(1)
        hold(0)
        for k in range(2, nch):
            send(k)
        forward(0)

        def rest():
            for k in range(1, nch):
                hold(k)
                forward(k)
            for k in range(nch):
                to_sib(ph, k).wait_send()

        return rest

    def reduce_end(ph, between=None):
        rows = pl.ds((ph % 2) * HALF, HALF)
        for k in range(nch):
            to_peer(ph, k).wait()
            total = (sx[ph % 2, k].astype(F32) + rx[ph % 4, k].astype(F32)).astype(BF)
            x[rows, chunk(1, k)] = (x[rows, chunk(1, k)].astype(F32) + total.astype(F32)).astype(BF)
            share(ph, k).start()
            if final(ph):
                keep(ph, k).start()
        if between is not None:
            between()
        for k in range(nch):
            share(ph, k).wait()

    def gate_up(layer, half):
        rows = pl.ds(half * HALF, HALF)
        h[...] = normed(x[rows, :].astype(F32), mnorm[layer:layer + 1, :].astype(F32))

        @pl.loop(0, ncol // GC)
        def _(n):
            if half == 0:
                for c in range(GC):
                    for cp in gu_copies(layer, n * GC + c):
                        cp.wait()
            wide = lambda ref: jnp.concatenate([ref[n * GC + c] for c in range(GC)], axis=1)
            g = jnp.dot(h[...], wide(wg), preferred_element_type=F32).astype(BF).astype(F32)
            u = jnp.dot(h[...], wide(wu), preferred_element_type=F32).astype(BF).astype(F32)
            cols = pl.ds(pl.multiple_of(n * GC * 128, GC * 128), GC * 128)
            act[:, cols] = (g * jax.nn.sigmoid(g) * u).astype(BF)

    def qkv_rope(half):
        rows = pl.ds(half * HALF, HALF)
        h[...] = normed(x[rows, :].astype(F32), anorm[1:2, :].astype(F32))

        full = jnp.dot(h[...], wqkv[...], preferred_element_type=F32).astype(BF)
        for n in range(qkv.shape[0]):
            qkv[n] = full[:, n * 256:(n + 1) * 256]

        cos_b = cs[rows, 0:128]
        sin_b = cs[rows, 128:256]

        def piece(n, i):
            return qkv[n, :, i * 128:i * 128 + 128].astype(F32)

        def rope(vec):
            return (vec * cos_b + pltpu.roll(vec, 64, 1) * sin_b).astype(BF)

        k_new = [rope(piece(heads // 2, i)) for i in range(2)]
        v_new = [piece(heads // 2 + 1, i) for i in range(2)]
        for i in range(2):
            new[i, rows, :] = k_new[i]
            new[2 + i, rows, :] = v_new[i].astype(BF)
        zero = jnp.zeros((HALF, 128), F32)
        for j in range(8):
            out_rows = pl.ds(j, HALF, stride=8)
            kv = 0 if j < heads // 2 else 1
            q_rows[out_rows, :] = rope(piece(j // 2, j % 2)).astype(F32) if j < heads else zero
            k_rows[out_rows, :] = k_new[kv].astype(F32)
            v_rows[out_rows, :] = v_new[kv]

    col = lax.broadcasted_iota(jnp.int32, (8, 256), 1)
    row = lax.broadcasted_iota(jnp.int32, (8, 256), 0)
    key_row = jnp.where((col & 1) == jnp.where(row >= heads // 2, 1, 0), col >> 1, 4096)
    scale = 128 ** -0.5

    def attend(half):
        pairs = range(SLOT)
        zero8 = jnp.zeros((8, 128), F32)
        steps = ncol // 2

        def rows8(i, p, b):
            return pl.ds(pl.multiple_of((i * 2 * SLOT + 2 * p + b) * 8, 8), 8)

        def both(ref, i, p):
            r = 2 * p % SLOT
            slot = 2 * i + 2 * p // SLOT
            return jnp.concatenate([ref[slot, r * 256:(r + 1) * 256, :], ref[slot, (r + 1) * 256:(r + 2) * 256, :]], axis=1)

        def score(i):
            for p in pairs:
                qa = q_rows[rows8(i, p, 0), :]
                qb = q_rows[rows8(i, p, 1), :]
                q2 = jnp.concatenate([jnp.concatenate([qa, zero8], axis=1), jnp.concatenate([zero8, qb], axis=1)], axis=0).astype(BF)
                s_buf[lax.rem(i, 2), p] = lax.dot_general(q2, both(wg, i, p), (((1,), (1,)), ((), ())), preferred_element_type=F32)

        def step(i, more):
            if more:
                for c in range(2):
                    kv_copies(half, 2 * i + 2 + c)[0].wait()
            for c in range(2):
                kv_copies(half, 2 * i + c)[1].wait()
            scores = [s_buf[lax.rem(i, 2), p] for p in pairs]
            if more:
                score(i + 1)
            weights, last = [], []
            for p in pairs:
                prod = jnp.concatenate([q_rows[rows8(i, p, b), :] * k_rows[rows8(i, p, b), :] for b in range(2)], axis=0)
                fresh = jnp.sum(prod, axis=-1, keepdims=True) * scale
                pos = [pos_ref[half * HALF + i * 2 * SLOT + 2 * p + b] for b in range(2)]
                before = jnp.concatenate([key_row < pos[0], key_row < pos[1]], axis=0)
                s = jnp.where(before, scores[p] * scale, NEG)
                peak = jnp.maximum(jnp.max(s, axis=-1, keepdims=True), fresh)
                e = jnp.exp(s - peak)
                e_new = jnp.exp(fresh - peak)
                inv = 1.0 / (jnp.sum(e, axis=-1, keepdims=True) + e_new)
                weights.append((e * inv).astype(BF))
                last.append((e_new * inv).astype(BF).astype(F32))
            outs = [jnp.dot(weights[p], both(wu, i, p), preferred_element_type=F32) for p in pairs]
            for p in pairs:
                o_rows[rows8(i, p, 0), :] = outs[p][0:8, 0:128] + last[p][0:8] * v_rows[rows8(i, p, 0), :]
                o_rows[rows8(i, p, 1), :] = outs[p][8:16, 128:256] + last[p][8:16] * v_rows[rows8(i, p, 1), :]
            for c in range(2):
                for cp in (kv_copies(1, 2 * i + c) if half == 0 else gu_copies(1, 2 * i + c)):
                    cp.start()

        for c in range(2):
            kv_copies(half, c)[0].wait()
        score(0)

        @pl.loop(0, steps - 1)
        def _(i):
            step(i, True)

        step(steps - 1, False)

        rows = pl.ds(half * HALF, HALF)
        for j in range(heads):
            att[rows, j * 128:(j + 1) * 128] = o_rows[pl.ds(j, HALF, stride=8), :].astype(BF)

    def att_half(half):
        return lambda: att[half * HALF:(half + 1) * HALF, :]

    att_copy.wait()
    x_copy.wait()
    reduce_start(0, att_half(0), wo, lambda side, k: wo_copy(0, side, k))()

    @pl.loop(0, ncol)
    def _(c):
        for cp in gu_copies(0, c):
            cp.start()

    wd_copy(0).start()
    for c in qkv_loads:
        c.start()
    rest = reduce_start(1, att_half(1), wo, None)
    for c in small:
        c.wait()

    @pl.loop(0, 2 * HALF // 8)
    def _(i):
        for b in range(8):
            r = i * 8 + b
            cs[pl.ds(r, 1), :] = table[pl.ds(pos_ref[r], 1), :]

    for half in range(2):
        reduce_end(half, rest)
        if half == 0:
            for k in range(nch):
                wo_copy(1, 0, k).start()
                wo_copy(1, 1, k).start()
        gate_up(0, half)
        if half == 0:
            wd_copy(0).wait()
        else:
            @pl.loop(0, ncol)
            def _(c):
                for cp in kv_copies(0, c):
                    cp.start()

        rest = reduce_start(2 + half, lambda: act[...], wd, None)
    for half in range(2):
        reduce_end(2 + half, rest)
        if half == 0:
            wd_copy(1).start()
            for c in qkv_loads:
                c.wait()
        qkv_rope(half)
        attend(half)
        rest = reduce_start(4 + half, att_half(half), wo, (lambda side, k: wo_copy(1, side, k)) if half == 0 else None)
    new_copy = pltpu.make_async_copy(new, new_hbm, isem.at[6])
    new_copy.start()
    for half in range(2):
        reduce_end(4 + half, rest)
        gate_up(1, half)
        if half == 0:
            wd_copy(1).wait()
        rest = reduce_start(6 + half, lambda: act[...], wd, None)
    reduce_end(6, rest)
    reduce_end(7)
    new_copy.wait()
    for half in range(2):
        for k in range(nch):
            keep(6 + half, k).wait()


def mega(positions, table, att, hidden, mnorm, anorm, wo, wg, wu, wd, wq, wk, wv, k_rows, v_rows):
    batch, dim = hidden.shape
    nch = dim // 2 // CW
    cols = wq.shape[2] + 2 * wk.shape[2]
    ncol = wg.shape[2] // 128
    anyspec = pl.BlockSpec(memory_space=pl.ANY)
    msg = lambda n: pltpu.VMEM((n, nch, HALF, CW), BF)
    sems = pltpu.SemaphoreType.DMA((8, nch))
    rows = pltpu.VMEM((HALF * 8, 128), F32)
    args = [positions, table, att, hidden, mnorm, anorm, wo, wg, wu, wd, wq, wk, wv, k_rows, v_rows]
    return pl.pallas_call(
        mega_kernel,
        out_shape=(jax.ShapeDtypeStruct((batch, dim), BF), jax.ShapeDtypeStruct((4, batch, 128), BF)),
        in_specs=[anyspec] * len(args),
        out_specs=(anyspec, anyspec),
        scratch_shapes=[
            pltpu.SMEM((batch,), jnp.int32), pltpu.VMEM(table.shape, F32), pltpu.VMEM((batch, table.shape[1]), F32),
            pltpu.VMEM(wo.shape[1:], BF), pltpu.VMEM((ncol, dim, 128), BF), pltpu.VMEM((ncol, dim, 128), BF), pltpu.VMEM(wd.shape[1:], BF),
            pltpu.VMEM((dim, cols), BF), pltpu.VMEM(att.shape, BF), pltpu.VMEM(hidden.shape, BF),
            pltpu.VMEM(mnorm.shape, BF), pltpu.VMEM(anorm.shape, BF),
            pltpu.VMEM((HALF, dim), BF), pltpu.VMEM((HALF, wd.shape[1]), BF), pltpu.VMEM((cols // 256, HALF, 256), BF),
            rows, rows, rows, rows, pltpu.VMEM((2, SLOT, 16, 256), F32), pltpu.VMEM((4, batch, 128), BF),
            pltpu.VMEM((nch, HALF, CW), F32), msg(2), msg(2), msg(4), msg(4),
            pltpu.SemaphoreType.DMA((2, nch)), pltpu.SemaphoreType.DMA((ncol,)), pltpu.SemaphoreType.DMA((ncol,)),
            pltpu.SemaphoreType.DMA((4,)), pltpu.SemaphoreType.DMA((7,)),
            sems, sems, sems, sems, sems, sems, pltpu.SemaphoreType.DMA((2, nch)),
        ],
        compiler_params=pltpu.CompilerParams(collective_id=0, has_side_effects=True, vmem_limit_bytes=67043328),
        name="mega",
    )(*args)


def solution(mesh):
    row_spec = P('dp', None)
    pos_spec = P('dp')
    cache_spec = P(None, 'dp', None, 'tp', None)
    norm_spec = P(None, None)
    col_spec = P(None, None, 'tp')
    split_rows = P(None, 'tp', None)

    def local_step(hidden, positions, k_cache, v_cache, attn_norm, w_query, w_key, w_value, w_out, mlp_norm, w_gate, w_up, w_down):
        cache_shape = k_cache.shape
        flat = (cache_shape[0], cache_shape[1], cache_shape[2] * cache_shape[3], cache_shape[4])
        k_flat, v_flat = k_cache.reshape(flat), v_cache.reshape(flat)
        table = jnp.asarray(rope_table(cache_shape[2], cache_shape[4]))
        source = (hidden, attn_norm, w_query, w_key, w_value)
        att, *caches = attention(0, positions, table, source, k_flat, v_flat, None, w_query.shape[2], w_key.shape[2])
        rows = (cache_shape[0], -1, cache_shape[4])
        hidden, new = mega(positions, table, att, hidden, mlp_norm, attn_norm, w_out, w_gate, w_up, w_down, w_query, w_key, w_value,
                           k_cache.reshape(rows), v_cache.reshape(rows))
        caches = write_rows(1, positions, new, k_flat, v_flat, caches)
        return hidden, caches[0].reshape(cache_shape), caches[1].reshape(cache_shape)

    return jax.shard_map(local_step, mesh=mesh, in_specs=(row_spec, pos_spec, cache_spec, cache_spec, norm_spec, col_spec, col_spec, col_spec, split_rows, norm_spec, col_spec, col_spec, split_rows), out_specs=(row_spec, cache_spec, cache_spec), check_vma=False)
```

```python
import functools
import math
import jax
import jax.numpy as jnp
import numpy as np
from jax import lax
from jax.experimental import pallas as pl
from jax.experimental.pallas import tpu as pltpu
from jax.sharding import PartitionSpec as P

BF = jnp.bfloat16
F32 = jnp.float32
MESH = pl.DeviceIdType.MESH
EPS = 1e-5
NEG = -1e30


def rope_table(rows, head_dim):
    half_dim = head_dim // 2
    inv_freq = np.power(np.float32(500000.0), -np.arange(half_dim, dtype=np.float32) * np.float32(2.0 / head_dim)).astype(np.float32)
    wavelen = (np.float32(2.0 * math.pi) / inv_freq).astype(np.float32)
    smooth = (np.float32(8192.0) / wavelen - np.float32(1.0)) / np.float32(3.0)
    blended = (np.float32(1.0) - smooth) * inv_freq / np.float32(8.0) + smooth * inv_freq
    scaled = np.where(wavelen < 2048.0, inv_freq, np.where(wavelen > 8192.0, inv_freq / np.float32(8.0), blended)).astype(np.float32)
    angles = np.arange(rows, dtype=np.float32)[:, None] * scaled[None, :]
    cos, sin = np.cos(angles.astype(np.float64)), np.sin(angles.astype(np.float64))
    return np.concatenate([cos, cos, -sin, sin], axis=-1).astype(np.float32)


def normed(x_f32, weight_f32):
    mean_sq = jnp.mean(x_f32 * x_f32, axis=-1, keepdims=True)
    return (x_f32 * lax.rsqrt(mean_sq + EPS) * weight_f32).astype(BF)


BLK = 16
HOLD = 6


def patch(kbuf, vbuf, k_rows, v_rows, pos_ref, i):
    seq_in_group = lax.broadcasted_iota(jnp.int32, (16, 128), 0) >> 1
    for b in range(BLK):
        pos = pos_ref[i * BLK + b]
        group = pl.ds(pl.multiple_of((pos >> 3) * 16, 16), 16)
        hit = seq_in_group == (pos & 7)
        rows = pl.ds(pl.multiple_of((i * BLK + b) * 8, 8), 8)
        for buf, new in ((kbuf, k_rows), (vbuf, v_rows)):
            new8 = new[rows, :]
            new16 = jnp.concatenate([new8, new8], axis=0)
            old16 = buf[i, b, group, :].astype(F32)
            buf[i, b, group, :] = jnp.where(hit, new16, old16).astype(BF)


def attn_kernel(layer, pos_hbm, table_hbm, x_hbm, norm_hbm, wq_hbm, wk_hbm, wv_hbm, k_hbm, v_hbm, att_hbm, ko_hbm, vo_hbm,
                pos_ref, table, cs, q_rows, k_rows, v_rows, o_rows, s_buf, att, kbuf, vbuf, x_buf, norm, w_buf, h_buf, sem, insem, outsem):
    nblk = kbuf.shape[0]
    batch = nblk * BLK
    heads = att.shape[1] // 128
    qcols = wq_hbm.shape[2]
    kcols = wk_hbm.shape[2]
    first = [pltpu.make_async_copy(pos_hbm, pos_ref, sem.at[0]), pltpu.make_async_copy(table_hbm, table, sem.at[1])]
    x_copies = [pltpu.make_async_copy(x_hbm, x_buf, sem.at[2]), pltpu.make_async_copy(norm_hbm, norm, sem.at[3])]
    w_copies = [
        pltpu.make_async_copy(wq_hbm.at[layer], w_buf.at[:, pl.ds(0, qcols)], sem.at[4]),
        pltpu.make_async_copy(wk_hbm.at[layer], w_buf.at[:, pl.ds(qcols, kcols)], sem.at[5]),
        pltpu.make_async_copy(wv_hbm.at[layer], w_buf.at[:, pl.ds(qcols + kcols, kcols)], sem.at[6]),
    ]
    for c in first + x_copies + w_copies:
        c.start()

    def in_copies(i):
        rows = pl.ds(i * BLK, BLK)
        return (pltpu.make_async_copy(k_hbm.at[layer, rows], kbuf.at[i], insem.at[0, i]),
                pltpu.make_async_copy(v_hbm.at[layer, rows], vbuf.at[i], insem.at[1, i]))

    def out_copies(i):
        rows = pl.ds(i * BLK, BLK)
        return (pltpu.make_async_copy(kbuf.at[i], ko_hbm.at[layer, rows], outsem.at[0, i]),
                pltpu.make_async_copy(vbuf.at[i], vo_hbm.at[layer, rows], outsem.at[1, i]))

    @pl.loop(0, nblk)
    def _(i):
        for c in in_copies(i):
            c.start()

    for c in first:
        c.wait()

    @pl.loop(0, batch // 8)
    def _(i):
        for b in range(8):
            r = i * 8 + b
            cs[pl.ds(r, 1), :] = table[pl.ds(pos_ref[r], 1), :]

    for c in x_copies:
        c.wait()
    h_buf[...] = normed(x_buf[...].astype(F32), norm[layer:layer + 1, :].astype(F32))
    cos_b = cs[:, 0:128]
    sin_b = cs[:, 128:256]
    for c in w_copies:
        c.wait()
    full = jnp.dot(h_buf[...], w_buf[...], preferred_element_type=F32).astype(BF)

    def piece(j):
        return full[:, j * 128:(j + 1) * 128].astype(F32)

    def rope(vec):
        return (vec * cos_b + pltpu.roll(vec, 64, 1) * sin_b).astype(BF).astype(F32)

    zero = jnp.zeros((batch, 128), F32)
    for j in range(8):
        q_rows[pl.ds(j, batch, stride=8), :] = rope(piece(j)) if j < heads else zero
    for h in range(2):
        k_vec = rope(piece(heads + h))
        v_vec = piece(heads + 2 + h)
        for r in range(4):
            k_rows[pl.ds(2 * r + h, batch, stride=8), :] = k_vec
            v_rows[pl.ds(2 * r + h, batch, stride=8), :] = v_vec

    col = lax.broadcasted_iota(jnp.int32, (8, 256), 1)
    row = lax.broadcasted_iota(jnp.int32, (8, 256), 0)
    key_row = jnp.where((col & 1) == jnp.where(row >= heads // 2, 1, 0), col >> 1, 4096)
    scale = 128 ** -0.5
    pairs = range(BLK // 2)
    zero8 = jnp.zeros((8, 128), F32)

    def both(buf, i, p):
        return jnp.concatenate([buf[i, 2 * p], buf[i, 2 * p + 1]], axis=1)

    def score(i):
        for p in pairs:
            qa, qb = [q_rows[pl.ds(pl.multiple_of((i * BLK + 2 * p + b) * 8, 8), 8), :] for b in range(2)]
            q2 = jnp.concatenate([jnp.concatenate([qa, zero8], axis=1), jnp.concatenate([zero8, qb], axis=1)], axis=0).astype(BF)
            s_buf[lax.rem(i, 2), p] = lax.dot_general(q2, both(kbuf, i, p), (((1,), (1,)), ((), ())), preferred_element_type=F32)

    def step(i, more):
        if more:
            for c in in_copies(i + 1):
                c.wait()
            patch(kbuf, vbuf, k_rows, v_rows, pos_ref, i + 1)
        scores = [s_buf[lax.rem(i, 2), p] for p in pairs]
        if more:
            score(i + 1)
        weights = []
        for p in pairs:
            first_row = i * BLK + 2 * p
            seen = jnp.concatenate([key_row <= pos_ref[first_row], key_row <= pos_ref[first_row + 1]], axis=0)
            s = jnp.where(seen, scores[p] * scale, NEG)
            e = jnp.exp(s - jnp.max(s, axis=-1, keepdims=True))
            weights.append((e * (1.0 / jnp.sum(e, axis=-1, keepdims=True))).astype(BF))
        outs = [jnp.dot(weights[p], both(vbuf, i, p), preferred_element_type=F32) for p in pairs]
        for p in pairs:
            o_rows[16 * p:16 * p + 8, :] = outs[p][0:8, 0:128]
            o_rows[16 * p + 8:16 * p + 16, :] = outs[p][8:16, 128:256]
        rows = pl.ds(pl.multiple_of(i * BLK, BLK), BLK)
        for j in range(heads):
            att[rows, j * 128:(j + 1) * 128] = o_rows[pl.ds(j, BLK, stride=8), :].astype(BF)

        @pl.when(i == HOLD)
        def _():
            @pl.loop(0, HOLD)
            def _(j):
                for c in out_copies(j):
                    c.start()

        @pl.when(i >= HOLD)
        def _():
            for c in out_copies(i):
                c.start()

    for c in in_copies(0):
        c.wait()
    patch(kbuf, vbuf, k_rows, v_rows, pos_ref, 0)
    score(0)

    @pl.loop(0, nblk - 1)
    def _(i):
        step(i, True)

    step(nblk - 1, False)
    att_copy = pltpu.make_async_copy(att, att_hbm, sem.at[7])
    att_copy.start()
    att_copy.wait()

    @pl.loop(0, nblk)
    def _(i):
        for c in out_copies(i):
            c.wait()


def attention(layer, positions, table, hidden, norm, wq, wk, wv, k_cache, v_cache):
    batch, dim = hidden.shape
    qcols = wq.shape[2]
    cols = qcols + 2 * wk.shape[2]
    nblk = batch // BLK
    hbm = pl.BlockSpec(memory_space=pltpu.HBM)
    rows = pltpu.VMEM((batch * 8, 128), F32)
    args = [positions, table, hidden, norm, wq, wk, wv, k_cache, v_cache]
    return pl.pallas_call(
        functools.partial(attn_kernel, layer),
        out_shape=(jax.ShapeDtypeStruct((batch, qcols), BF),
                   jax.ShapeDtypeStruct(k_cache.shape, BF), jax.ShapeDtypeStruct(v_cache.shape, BF)),
        in_specs=[hbm] * len(args),
        out_specs=(hbm, hbm, hbm),
        scratch_shapes=[
            pltpu.SMEM((batch,), jnp.int32),
            pltpu.VMEM(table.shape, F32),
            pltpu.VMEM((batch, table.shape[1]), F32),
            rows, rows, rows,
            pltpu.VMEM((BLK * 8, 128), F32),
            pltpu.VMEM((2, BLK // 2, 16, 256), F32),
            pltpu.VMEM((batch, qcols), BF),
            pltpu.VMEM((nblk, BLK) + k_cache.shape[2:], BF),
            pltpu.VMEM((nblk, BLK) + v_cache.shape[2:], BF),
            pltpu.VMEM(hidden.shape, BF), pltpu.VMEM(norm.shape, BF), pltpu.VMEM((dim, cols), BF), pltpu.VMEM(hidden.shape, BF),
            pltpu.SemaphoreType.DMA((8,)),
            pltpu.SemaphoreType.DMA((2, nblk)),
            pltpu.SemaphoreType.DMA((2, nblk)),
        ],
        compiler_params=pltpu.CompilerParams(vmem_limit_bytes=62 * 2**20),
        cost_estimate=pl.CostEstimate(flops=2 * batch * dim * cols, bytes_accessed=76 * 2**20, transcendentals=0),
        name=f"attn{layer}",
    )(*args)


COPY_HOLD = 11


def write_kernel(layer, pos_hbm, new_hbm, k_hbm, v_hbm, k_prev, v_prev, ko_hbm, vo_hbm, pos_ref, new, k_rows, v_rows, kbuf, vbuf, sem, insem, outsem):
    nblk = kbuf.shape[0]
    batch = nblk * BLK
    first = [pltpu.make_async_copy(pos_hbm, pos_ref, sem.at[0]), pltpu.make_async_copy(new_hbm.at[0], new, sem.at[1])]
    for c in first:
        c.start()

    def in_copies(i):
        rows = pl.ds(i * BLK, BLK)
        return (pltpu.make_async_copy(k_hbm.at[layer, rows], kbuf.at[i], insem.at[0, i]),
                pltpu.make_async_copy(v_hbm.at[layer, rows], vbuf.at[i], insem.at[1, i]))

    def out_copies(i):
        rows = pl.ds(i * BLK, BLK)
        return (pltpu.make_async_copy(kbuf.at[i], ko_hbm.at[layer, rows], outsem.at[0, i]),
                pltpu.make_async_copy(vbuf.at[i], vo_hbm.at[layer, rows], outsem.at[1, i]))

    @pl.loop(0, nblk)
    def _(i):
        for c in in_copies(i):
            c.start()

    for c in first:
        c.wait()
    for h in range(2):
        k_vec = new[h].astype(F32)
        v_vec = new[2 + h].astype(F32)
        for r in range(4):
            k_rows[pl.ds(2 * r + h, batch, stride=8), :] = k_vec
            v_rows[pl.ds(2 * r + h, batch, stride=8), :] = v_vec

    @pl.loop(0, nblk)
    def _(i):
        for c in in_copies(i):
            c.wait()
        patch(kbuf, vbuf, k_rows, v_rows, pos_ref, i)

        @pl.when(i == COPY_HOLD)
        def _():
            @pl.loop(0, COPY_HOLD)
            def _(j):
                for c in out_copies(j):
                    c.start()

        @pl.when(i >= COPY_HOLD)
        def _():
            for c in out_copies(i):
                c.start()

    @pl.loop(0, nblk)
    def _(i):
        for c in out_copies(i):
            c.wait()


def write_rows(layer, positions, new, k_cache, v_cache, prev):
    batch = positions.shape[0]
    nblk = batch // BLK
    anyspec = pl.BlockSpec(memory_space=pltpu.HBM)
    return pl.pallas_call(
        functools.partial(write_kernel, layer),
        out_shape=(jax.ShapeDtypeStruct(k_cache.shape, BF), jax.ShapeDtypeStruct(v_cache.shape, BF)),
        in_specs=[anyspec] * 6,
        out_specs=(anyspec, anyspec),
        scratch_shapes=[
            pltpu.SMEM((batch,), jnp.int32),
            pltpu.VMEM(new.shape[1:], BF),
            pltpu.VMEM((batch * 8, 128), F32),
            pltpu.VMEM((batch * 8, 128), F32),
            pltpu.VMEM((nblk, BLK) + k_cache.shape[2:], BF),
            pltpu.VMEM((nblk, BLK) + v_cache.shape[2:], BF),
            pltpu.SemaphoreType.DMA((2,)),
            pltpu.SemaphoreType.DMA((2, nblk)),
            pltpu.SemaphoreType.DMA((2, nblk)),
        ],
        input_output_aliases={4: 0, 5: 1},
        compiler_params=pltpu.CompilerParams(vmem_limit_bytes=50 * 2**20),
        cost_estimate=pl.CostEstimate(flops=0, bytes_accessed=67 * 2**20, transcendentals=0),
        name="write_rows",
    )(positions, new, k_cache, v_cache, *prev)


CW = 512
HALF = 128
GC = 4
SPARE = 64
SLOT = 8


def mega_kernel(pos_hbm, table_hbm, att_hbm, x_hbm, mnorm_hbm, anorm_hbm, wo_hbm, wg_hbm, wu_hbm, wd_hbm, wq_hbm, wk_hbm, wv_hbm, k_hbm, v_hbm,
                out_hbm, new_hbm,
                pos_ref, table, cs, wo, wg, wu, wd, wqkv, att, x, mnorm, anorm, h, act, qkv, q_rows, k_rows, v_rows, o_rows, s_buf, new,
                own, sd, sx, rd, rx,
                wosem, gsem, usem, wsem, isem, hsem, sd_sem, sx_sem, sg_sem, rd_sem, rx_sem, ra_sem, osem):
    dim = x.shape[1]
    nch = dim // 2 // CW
    ncol = wg.shape[0]
    qcols = wq_hbm.shape[2]
    kcols = wk_hbm.shape[2]
    heads = qcols // 128
    tp = lax.axis_index("tp")
    core = lax.rem(tp, 2)
    sib = tp + 1 - 2 * core
    peer = lax.rem(tp + 2, 4)
    mine = pl.multiple_of(core * (dim // 2), CW)
    theirs = pl.multiple_of((1 - core) * (dim // 2), CW)

    def chunk(side, k):
        return pl.ds(pl.multiple_of((theirs, mine)[side] + k * CW, CW), CW)

    def wo_copy(layer, side, k):
        return pltpu.make_async_copy(wo_hbm.at[layer, :, chunk(side, k)], wo.at[:, chunk(side, k)], wosem.at[side, k])

    def gu_copies(layer, c):
        cols = pl.ds(pl.multiple_of(c * 128, 128), 128)
        return (pltpu.make_async_copy(wg_hbm.at[layer, :, cols], wg.at[c], gsem.at[c]),
                pltpu.make_async_copy(wu_hbm.at[layer, :, cols], wu.at[c], usem.at[c]))

    def kv_copies(half, c):
        src = pl.ds(pl.multiple_of((half * HALF + c * SLOT) * 256, 2048), SLOT * 256)
        dst = pl.ds(0, SLOT * 256)
        return (pltpu.make_async_copy(k_hbm.at[1, src], wg.at[c, dst], gsem.at[c]),
                pltpu.make_async_copy(v_hbm.at[1, src], wu.at[c, dst], usem.at[c]))

    def wd_copy(layer):
        return pltpu.make_async_copy(wd_hbm.at[layer], wd, wsem.at[0])

    def half_copy(which, half):
        rows = pl.ds(half * HALF, HALF)
        src, dst = ((att_hbm, att), (x_hbm, x))[which]
        return pltpu.make_async_copy(src.at[rows], dst.at[rows], hsem.at[which, half])

    small = [pltpu.make_async_copy(mnorm_hbm, mnorm, isem.at[2]), pltpu.make_async_copy(anorm_hbm, anorm, isem.at[3]),
             pltpu.make_async_copy(pos_hbm, pos_ref, isem.at[4]), pltpu.make_async_copy(table_hbm, table, isem.at[5])]
    qkv_loads = [
        pltpu.make_async_copy(wq_hbm.at[1], wqkv.at[:, pl.ds(0, qcols)], wsem.at[1]),
        pltpu.make_async_copy(wk_hbm.at[1], wqkv.at[:, pl.ds(qcols, kcols)], wsem.at[2]),
        pltpu.make_async_copy(wv_hbm.at[1], wqkv.at[:, pl.ds(qcols + kcols, kcols)], wsem.at[3]),
    ]
    half_copy(0, 0).start()
    wo_copy(0, 0, 0).start()
    half_copy(1, 0).start()
    wo_copy(0, 0, 1).start()
    wo_copy(0, 1, 0).start()
    for k in range(2, nch):
        wo_copy(0, 0, k).start()
    for k in range(1, nch):
        wo_copy(0, 1, k).start()
    half_copy(0, 1).start()
    half_copy(1, 1).start()
    for c in small:
        c.start()

    barrier = pltpu.get_barrier_semaphore()
    for other in (sib, peer):
        pl.semaphore_signal(barrier, inc=1, device_id={"tp": other}, device_id_type=MESH)
    pl.semaphore_wait(barrier, 2)

    def to_sib(ph, k):
        return pltpu.make_async_remote_copy(sd.at[ph % 2, k], rd.at[ph % 4, k], sd_sem.at[ph, k], rd_sem.at[ph, k],
                                            device_id={"tp": sib}, device_id_type=MESH)

    def to_peer(ph, k):
        return pltpu.make_async_remote_copy(sx.at[ph % 2, k], rx.at[ph % 4, k], sx_sem.at[ph, k], rx_sem.at[ph, k],
                                            device_id={"tp": peer}, device_id_type=MESH)

    def final(ph):
        return ph >= 6

    def share(ph, k):
        rows = pl.ds((ph % 2) * HALF, HALF)
        dst = out_hbm if final(ph) else x
        return pltpu.make_async_remote_copy(x.at[rows, chunk(1, k)], dst.at[rows, chunk(1, k)], sg_sem.at[ph, k], ra_sem.at[ph, k],
                                            device_id={"tp": sib}, device_id_type=MESH)

    def keep(ph, k):
        rows = pl.ds((ph % 2) * HALF, HALF)
        return pltpu.make_async_copy(x.at[rows, chunk(1, k)], out_hbm.at[rows, chunk(1, k)], osem.at[ph % 2, k])

    def reduce_start(ph, lhs, w_ref, load):
        def dot(side, k):
            if load is not None:
                load(side, k).wait()
            return jnp.dot(lhs(), w_ref[:, chunk(side, k)], preferred_element_type=F32)

        def send(k):
            sd[ph % 2, k] = dot(0, k).astype(BF)
            to_sib(ph, k).start()

        def hold(k):
            own[k] = dot(1, k)

        def forward(k):
            to_sib(ph, k).wait_recv()
            sx[ph % 2, k] = (own[k] + rd[ph % 4, k].astype(F32)).astype(BF)
            to_peer(ph, k).start()

        send(0)
        send(1)
        hold(0)
        for k in range(2, nch):
            send(k)
        forward(0)

        def rest():
            for k in range(1, nch):
                hold(k)
                forward(k)
            for k in range(nch):
                to_sib(ph, k).wait_send()

        return rest

    def reduce_end(ph, between=None):
        rows = pl.ds((ph % 2) * HALF, HALF)
        for k in range(nch):
            to_peer(ph, k).wait()
            total = (sx[ph % 2, k].astype(F32) + rx[ph % 4, k].astype(F32)).astype(BF)
            x[rows, chunk(1, k)] = (x[rows, chunk(1, k)].astype(F32) + total.astype(F32)).astype(BF)
            share(ph, k).start()
            if final(ph):
                keep(ph, k).start()
        if between is not None:
            between()
        for k in range(nch):
            share(ph, k).wait()

    def gate_up(layer, half):
        rows = pl.ds(half * HALF, HALF)
        h[...] = normed(x[rows, :].astype(F32), mnorm[layer:layer + 1, :].astype(F32))

        @pl.loop(0, ncol // GC)
        def _(n):
            if half == 0:
                for c in range(GC):
                    for cp in gu_copies(layer, n * GC + c):
                        cp.wait()
            wide = lambda ref: jnp.concatenate([ref[n * GC + c] for c in range(GC)], axis=1)
            g = jnp.dot(h[...], wide(wg), preferred_element_type=F32).astype(BF).astype(F32)
            u = jnp.dot(h[...], wide(wu), preferred_element_type=F32).astype(BF).astype(F32)
            cols = pl.ds(pl.multiple_of(n * GC * 128, GC * 128), GC * 128)
            act[:, cols] = (g * jax.nn.sigmoid(g) * u).astype(BF)

    def qkv_rope(half):
        rows = pl.ds(half * HALF, HALF)
        h[...] = normed(x[rows, :].astype(F32), anorm[1:2, :].astype(F32))

        full = jnp.dot(h[...], wqkv[...], preferred_element_type=F32).astype(BF)
        for n in range(qkv.shape[0]):
            qkv[n] = full[:, n * 256:(n + 1) * 256]

        cos_b = cs[rows, 0:128]
        sin_b = cs[rows, 128:256]

        def piece(n, i):
            return qkv[n, :, i * 128:i * 128 + 128].astype(F32)

        def rope(vec):
            return (vec * cos_b + pltpu.roll(vec, 64, 1) * sin_b).astype(BF)

        k_new = [rope(piece(heads // 2, i)) for i in range(2)]
        v_new = [piece(heads // 2 + 1, i) for i in range(2)]
        for i in range(2):
            new[i, rows, :] = k_new[i]
            new[2 + i, rows, :] = v_new[i].astype(BF)
        zero = jnp.zeros((HALF, 128), F32)
        for j in range(8):
            out_rows = pl.ds(j, HALF, stride=8)
            kv = 0 if j < heads // 2 else 1
            q_rows[out_rows, :] = rope(piece(j // 2, j % 2)).astype(F32) if j < heads else zero
            k_rows[out_rows, :] = k_new[kv].astype(F32)
            v_rows[out_rows, :] = v_new[kv]

    col = lax.broadcasted_iota(jnp.int32, (8, 256), 1)
    row = lax.broadcasted_iota(jnp.int32, (8, 256), 0)
    key_row = jnp.where((col & 1) == jnp.where(row >= heads // 2, 1, 0), col >> 1, 4096)
    scale = 128 ** -0.5

    def attend(half):
        pairs = range(SLOT)
        zero8 = jnp.zeros((8, 128), F32)
        steps = ncol // 2

        def rows8(i, p, b):
            return pl.ds(pl.multiple_of((i * 2 * SLOT + 2 * p + b) * 8, 8), 8)

        def both(ref, i, p):
            r = 2 * p % SLOT
            slot = 2 * i + 2 * p // SLOT
            return jnp.concatenate([ref[slot, r * 256:(r + 1) * 256, :], ref[slot, (r + 1) * 256:(r + 2) * 256, :]], axis=1)

        def score(i):
            for p in pairs:
                qa = q_rows[rows8(i, p, 0), :]
                qb = q_rows[rows8(i, p, 1), :]
                q2 = jnp.concatenate([jnp.concatenate([qa, zero8], axis=1), jnp.concatenate([zero8, qb], axis=1)], axis=0).astype(BF)
                s_buf[lax.rem(i, 2), p] = lax.dot_general(q2, both(wg, i, p), (((1,), (1,)), ((), ())), preferred_element_type=F32)

        def step(i, more):
            if more:
                for c in range(2):
                    kv_copies(half, 2 * i + 2 + c)[0].wait()
            for c in range(2):
                kv_copies(half, 2 * i + c)[1].wait()
            scores = [s_buf[lax.rem(i, 2), p] for p in pairs]
            if more:
                score(i + 1)
            weights, last = [], []
            for p in pairs:
                prod = jnp.concatenate([q_rows[rows8(i, p, b), :] * k_rows[rows8(i, p, b), :] for b in range(2)], axis=0)
                fresh = jnp.sum(prod, axis=-1, keepdims=True) * scale
                pos = [pos_ref[half * HALF + i * 2 * SLOT + 2 * p + b] for b in range(2)]
                before = jnp.concatenate([key_row < pos[0], key_row < pos[1]], axis=0)
                s = jnp.where(before, scores[p] * scale, NEG)
                peak = jnp.maximum(jnp.max(s, axis=-1, keepdims=True), fresh)
                e = jnp.exp(s - peak)
                e_new = jnp.exp(fresh - peak)
                inv = 1.0 / (jnp.sum(e, axis=-1, keepdims=True) + e_new)
                weights.append((e * inv).astype(BF))
                last.append((e_new * inv).astype(BF).astype(F32))
            outs = [jnp.dot(weights[p], both(wu, i, p), preferred_element_type=F32) for p in pairs]
            for p in pairs:
                o_rows[rows8(i, p, 0), :] = outs[p][0:8, 0:128] + last[p][0:8] * v_rows[rows8(i, p, 0), :]
                o_rows[rows8(i, p, 1), :] = outs[p][8:16, 128:256] + last[p][8:16] * v_rows[rows8(i, p, 1), :]
            for c in range(2):
                for cp in (kv_copies(1, 2 * i + c) if half == 0 else gu_copies(1, 2 * i + c)):
                    cp.start()

        for c in range(2):
            kv_copies(half, c)[0].wait()
        score(0)

        @pl.loop(0, steps - 1)
        def _(i):
            step(i, True)

        step(steps - 1, False)

        rows = pl.ds(half * HALF, HALF)
        for j in range(heads):
            att[rows, j * 128:(j + 1) * 128] = o_rows[pl.ds(j, HALF, stride=8), :].astype(BF)

    def att_half(half):
        return lambda: att[half * HALF:(half + 1) * HALF, :]

    half_copy(0, 0).wait()
    half_copy(1, 0).wait()
    reduce_start(0, att_half(0), wo, lambda side, k: wo_copy(0, side, k))()

    @pl.loop(0, ncol)
    def _(c):
        for cp in gu_copies(0, c):
            cp.start()

    wd_copy(0).start()
    for c in qkv_loads:
        c.start()
    half_copy(0, 1).wait()
    half_copy(1, 1).wait()
    rest = reduce_start(1, att_half(1), wo, None)
    for c in small:
        c.wait()

    @pl.loop(0, 2 * HALF // 8)
    def _(i):
        for b in range(8):
            r = i * 8 + b
            cs[pl.ds(r, 1), :] = table[pl.ds(pos_ref[r], 1), :]

    for half in range(2):
        reduce_end(half, rest)
        if half == 0:
            for k in range(nch):
                wo_copy(1, 0, k).start()
                wo_copy(1, 1, k).start()
        gate_up(0, half)
        if half == 0:
            wd_copy(0).wait()
        else:
            @pl.loop(0, ncol)
            def _(c):
                for cp in kv_copies(0, c):
                    cp.start()

        rest = reduce_start(2 + half, lambda: act[...], wd, None)
    for half in range(2):
        reduce_end(2 + half, rest)
        if half == 0:
            wd_copy(1).start()
            for c in qkv_loads:
                c.wait()
        qkv_rope(half)
        attend(half)
        rest = reduce_start(4 + half, att_half(half), wo, (lambda side, k: wo_copy(1, side, k)) if half == 0 else None)
    new_copy = pltpu.make_async_copy(new, new_hbm.at[0], isem.at[6])
    new_copy.start()
    for half in range(2):
        reduce_end(4 + half, rest)
        gate_up(1, half)
        if half == 0:
            wd_copy(1).wait()
        rest = reduce_start(6 + half, lambda: act[...], wd, None)
    reduce_end(6, rest)
    reduce_end(7)
    new_copy.wait()
    for half in range(2):
        for k in range(nch):
            keep(6 + half, k).wait()


def mega(positions, table, att, hidden, mnorm, anorm, wo, wg, wu, wd, wq, wk, wv, k_rows, v_rows):
    batch, dim = hidden.shape
    nch = dim // 2 // CW
    cols = wq.shape[2] + 2 * wk.shape[2]
    ncol = wg.shape[2] // 128
    anyspec = pl.BlockSpec(memory_space=pl.ANY)
    msg = lambda n: pltpu.VMEM((n, nch, HALF, CW), BF)
    sems = pltpu.SemaphoreType.DMA((8, nch))
    rows = pltpu.VMEM((HALF * 8, 128), F32)
    args = [positions, table, att, hidden, mnorm, anorm, wo, wg, wu, wd, wq, wk, wv, k_rows, v_rows]
    return pl.pallas_call(
        mega_kernel,
        out_shape=(jax.ShapeDtypeStruct((batch, dim), BF), jax.ShapeDtypeStruct((SPARE, 4, batch, 128), BF)),
        in_specs=[anyspec] * len(args),
        out_specs=(anyspec, anyspec),
        scratch_shapes=[
            pltpu.SMEM((batch,), jnp.int32), pltpu.VMEM(table.shape, F32), pltpu.VMEM((batch, table.shape[1]), F32),
            pltpu.VMEM(wo.shape[1:], BF), pltpu.VMEM((ncol, dim, 128), BF), pltpu.VMEM((ncol, dim, 128), BF), pltpu.VMEM(wd.shape[1:], BF),
            pltpu.VMEM((dim, cols), BF), pltpu.VMEM(att.shape, BF), pltpu.VMEM(hidden.shape, BF),
            pltpu.VMEM(mnorm.shape, BF), pltpu.VMEM(anorm.shape, BF),
            pltpu.VMEM((HALF, dim), BF), pltpu.VMEM((HALF, wd.shape[1]), BF), pltpu.VMEM((cols // 256, HALF, 256), BF),
            rows, rows, rows, rows, pltpu.VMEM((2, SLOT, 16, 256), F32), pltpu.VMEM((4, batch, 128), BF),
            pltpu.VMEM((nch, HALF, CW), F32), msg(2), msg(2), msg(4), msg(4),
            pltpu.SemaphoreType.DMA((2, nch)), pltpu.SemaphoreType.DMA((ncol,)), pltpu.SemaphoreType.DMA((ncol,)),
            pltpu.SemaphoreType.DMA((4,)), pltpu.SemaphoreType.DMA((7,)), pltpu.SemaphoreType.DMA((2, 2)),
            sems, sems, sems, sems, sems, sems, pltpu.SemaphoreType.DMA((2, nch)),
        ],
        compiler_params=pltpu.CompilerParams(collective_id=0, has_side_effects=True, vmem_limit_bytes=67043328),
        name="mega",
    )(*args)


def solution(mesh):
    row_spec = P('dp', None)
    pos_spec = P('dp')
    cache_spec = P(None, 'dp', None, 'tp', None)
    norm_spec = P(None, None)
    col_spec = P(None, None, 'tp')
    split_rows = P(None, 'tp', None)

    def local_step(hidden, positions, k_cache, v_cache, attn_norm, w_query, w_key, w_value, w_out, mlp_norm, w_gate, w_up, w_down):
        cache_shape = k_cache.shape
        flat = (cache_shape[0], cache_shape[1], cache_shape[2] * cache_shape[3], cache_shape[4])
        k_flat, v_flat = k_cache.reshape(flat), v_cache.reshape(flat)
        table = jnp.asarray(rope_table(cache_shape[2], cache_shape[4]))
        att, *caches = attention(0, positions, table, hidden, attn_norm, w_query, w_key, w_value, k_flat, v_flat)
        rows = (cache_shape[0], -1, cache_shape[4])
        hidden, new = mega(positions, table, att, hidden, mlp_norm, attn_norm, w_out, w_gate, w_up, w_down, w_query, w_key, w_value,
                           k_cache.reshape(rows), v_cache.reshape(rows))
        caches = write_rows(1, positions, new, k_flat, v_flat, caches)
        return hidden, caches[0].reshape(cache_shape), caches[1].reshape(cache_shape)

    return jax.shard_map(local_step, mesh=mesh, in_specs=(row_spec, pos_spec, cache_spec, cache_spec, norm_spec, col_spec, col_spec, col_spec, split_rows, norm_spec, col_spec, col_spec, split_rows), out_specs=(row_spec, cache_spec, cache_spec), check_vma=False)
```

```python
import functools
import math
import jax
import jax.numpy as jnp
import numpy as np
from jax import lax
from jax.experimental import pallas as pl
from jax.experimental.pallas import tpu as pltpu
from jax.sharding import PartitionSpec as P

BF = jnp.bfloat16
F32 = jnp.float32
MESH = pl.DeviceIdType.MESH
EPS = 1e-5
NEG = -1e30


def rope_table(rows, head_dim):
    half_dim = head_dim // 2
    inv_freq = np.power(np.float32(500000.0), -np.arange(half_dim, dtype=np.float32) * np.float32(2.0 / head_dim)).astype(np.float32)
    wavelen = (np.float32(2.0 * math.pi) / inv_freq).astype(np.float32)
    smooth = (np.float32(8192.0) / wavelen - np.float32(1.0)) / np.float32(3.0)
    blended = (np.float32(1.0) - smooth) * inv_freq / np.float32(8.0) + smooth * inv_freq
    scaled = np.where(wavelen < 2048.0, inv_freq, np.where(wavelen > 8192.0, inv_freq / np.float32(8.0), blended)).astype(np.float32)
    angles = np.arange(rows, dtype=np.float32)[:, None] * scaled[None, :]
    cos, sin = np.cos(angles.astype(np.float64)), np.sin(angles.astype(np.float64))
    return np.concatenate([cos, cos, -sin, sin], axis=-1).astype(np.float32)


def normed(x_f32, weight_f32):
    mean_sq = jnp.mean(x_f32 * x_f32, axis=-1, keepdims=True)
    return (x_f32 * lax.rsqrt(mean_sq + EPS) * weight_f32).astype(BF)


BLK = 16
ROOM = 1 << 23
HOLD = 6


def patch(kbuf, vbuf, k_rows, v_rows, pos_ref, i):
    seq_in_group = lax.broadcasted_iota(jnp.int32, (16, 128), 0) >> 1
    for b in range(BLK):
        pos = pos_ref[i * BLK + b]
        group = pl.ds(pl.multiple_of((pos >> 3) * 16, 16), 16)
        hit = seq_in_group == (pos & 7)
        rows = pl.ds(pl.multiple_of((i * BLK + b) * 8, 8), 8)
        for buf, new in ((kbuf, k_rows), (vbuf, v_rows)):
            new8 = new[rows, :]
            new16 = jnp.concatenate([new8, new8], axis=0)
            old16 = buf[i, b, group, :].astype(F32)
            buf[i, b, group, :] = jnp.where(hit, new16, old16).astype(BF)


def attn_kernel(layer, pos_hbm, table_hbm, x_hbm, norm_hbm, wq_hbm, wk_hbm, wv_hbm, k_hbm, v_hbm, att_hbm, ko_hbm, vo_hbm, where_hbm,
                pos_ref, table, cs, q_rows, k_rows, v_rows, o_rows, s_buf, att, kbuf, vbuf, x_buf, norm, w_buf, h_buf, sem, insem, outsem):
    nblk = kbuf.shape[0]
    batch = nblk * BLK
    heads = att.shape[1] // 128
    qcols = wq_hbm.shape[2]
    kcols = wk_hbm.shape[2]
    first = [pltpu.make_async_copy(pos_hbm, pos_ref, sem.at[0]), pltpu.make_async_copy(table_hbm, table, sem.at[1])]
    x_copies = [pltpu.make_async_copy(x_hbm, x_buf, sem.at[2]), pltpu.make_async_copy(norm_hbm, norm, sem.at[3])]
    w_copies = [
        pltpu.make_async_copy(wq_hbm.at[layer], w_buf.at[:, pl.ds(0, qcols)], sem.at[4]),
        pltpu.make_async_copy(wk_hbm.at[layer], w_buf.at[:, pl.ds(qcols, kcols)], sem.at[5]),
        pltpu.make_async_copy(wv_hbm.at[layer], w_buf.at[:, pl.ds(qcols + kcols, kcols)], sem.at[6]),
    ]
    for c in first + x_copies + w_copies:
        c.start()

    def in_copies(i):
        rows = pl.ds(i * BLK, BLK)
        return (pltpu.make_async_copy(k_hbm.at[layer, rows], kbuf.at[i], insem.at[0, i]),
                pltpu.make_async_copy(v_hbm.at[layer, rows], vbuf.at[i], insem.at[1, i]))

    def out_copies(i):
        rows = pl.ds(i * BLK, BLK)
        return (pltpu.make_async_copy(kbuf.at[i], ko_hbm.at[layer, rows], outsem.at[0, i]),
                pltpu.make_async_copy(vbuf.at[i], vo_hbm.at[layer, rows], outsem.at[1, i]))

    @pl.loop(0, nblk)
    def _(i):
        for c in in_copies(i):
            c.start()

    for c in first:
        c.wait()

    @pl.loop(0, batch // 8)
    def _(i):
        for b in range(8):
            r = i * 8 + b
            cs[pl.ds(r, 1), :] = table[pl.ds(pos_ref[r], 1), :]

    for c in x_copies:
        c.wait()
    h_buf[...] = normed(x_buf[...].astype(F32), norm[layer:layer + 1, :].astype(F32))
    cos_b = cs[:, 0:128]
    sin_b = cs[:, 128:256]
    for c in w_copies:
        c.wait()
    full = jnp.dot(h_buf[...], w_buf[...], preferred_element_type=F32).astype(BF)

    def piece(j):
        return full[:, j * 128:(j + 1) * 128].astype(F32)

    def rope(vec):
        return (vec * cos_b + pltpu.roll(vec, 64, 1) * sin_b).astype(BF).astype(F32)

    zero = jnp.zeros((batch, 128), F32)
    for j in range(8):
        q_rows[pl.ds(j, batch, stride=8), :] = rope(piece(j)) if j < heads else zero
    for h in range(2):
        k_vec = rope(piece(heads + h))
        v_vec = piece(heads + 2 + h)
        for r in range(4):
            k_rows[pl.ds(2 * r + h, batch, stride=8), :] = k_vec
            v_rows[pl.ds(2 * r + h, batch, stride=8), :] = v_vec

    col = lax.broadcasted_iota(jnp.int32, (8, 256), 1)
    row = lax.broadcasted_iota(jnp.int32, (8, 256), 0)
    key_row = jnp.where((col & 1) == jnp.where(row >= heads // 2, 1, 0), col >> 1, 4096)
    scale = 128 ** -0.5
    pairs = range(BLK // 2)
    zero8 = jnp.zeros((8, 128), F32)

    def both(buf, i, p):
        return jnp.concatenate([buf[i, 2 * p], buf[i, 2 * p + 1]], axis=1)

    def score(i):
        for p in pairs:
            qa, qb = [q_rows[pl.ds(pl.multiple_of((i * BLK + 2 * p + b) * 8, 8), 8), :] for b in range(2)]
            q2 = jnp.concatenate([jnp.concatenate([qa, zero8], axis=1), jnp.concatenate([zero8, qb], axis=1)], axis=0).astype(BF)
            s_buf[lax.rem(i, 2), p] = lax.dot_general(q2, both(kbuf, i, p), (((1,), (1,)), ((), ())), preferred_element_type=F32)

    def step(i, more):
        if more:
            for c in in_copies(i + 1):
                c.wait()
            patch(kbuf, vbuf, k_rows, v_rows, pos_ref, i + 1)
        scores = [s_buf[lax.rem(i, 2), p] for p in pairs]
        if more:
            score(i + 1)
        weights = []
        for p in pairs:
            first_row = i * BLK + 2 * p
            seen = jnp.concatenate([key_row <= pos_ref[first_row], key_row <= pos_ref[first_row + 1]], axis=0)
            s = jnp.where(seen, scores[p] * scale, NEG)
            e = jnp.exp(s - jnp.max(s, axis=-1, keepdims=True))
            weights.append((e * (1.0 / jnp.sum(e, axis=-1, keepdims=True))).astype(BF))
        outs = [jnp.dot(weights[p], both(vbuf, i, p), preferred_element_type=F32) for p in pairs]
        for p in pairs:
            o_rows[16 * p:16 * p + 8, :] = outs[p][0:8, 0:128]
            o_rows[16 * p + 8:16 * p + 16, :] = outs[p][8:16, 128:256]
        rows = pl.ds(pl.multiple_of(i * BLK, BLK), BLK)
        for j in range(heads):
            att[rows, j * 128:(j + 1) * 128] = o_rows[pl.ds(j, BLK, stride=8), :].astype(BF)

        @pl.when(i == HOLD)
        def _():
            @pl.loop(0, HOLD)
            def _(j):
                for c in out_copies(j):
                    c.start()

        @pl.when(i >= HOLD)
        def _():
            for c in out_copies(i):
                c.start()

    for c in in_copies(0):
        c.wait()
    patch(kbuf, vbuf, k_rows, v_rows, pos_ref, 0)
    score(0)

    @pl.loop(0, nblk - 1)
    def _(i):
        step(i, True)

    step(nblk - 1, False)
    results = [pltpu.make_async_copy(att, att_hbm, sem.at[7]), pltpu.make_async_copy(pos_ref, where_hbm.at[pl.ds(0, batch)], sem.at[8])]
    for c in results:
        c.start()
    for c in results:
        c.wait()

    @pl.loop(0, nblk)
    def _(i):
        for c in out_copies(i):
            c.wait()


def attention(layer, positions, table, hidden, norm, wq, wk, wv, k_cache, v_cache):
    batch, dim = hidden.shape
    qcols = wq.shape[2]
    cols = qcols + 2 * wk.shape[2]
    nblk = batch // BLK
    hbm = pl.BlockSpec(memory_space=pltpu.HBM)
    rows = pltpu.VMEM((batch * 8, 128), F32)
    args = [positions, table, hidden, norm, wq, wk, wv, k_cache, v_cache]
    return pl.pallas_call(
        functools.partial(attn_kernel, layer),
        out_shape=(jax.ShapeDtypeStruct((batch, qcols), BF),
                   jax.ShapeDtypeStruct(k_cache.shape, BF), jax.ShapeDtypeStruct(v_cache.shape, BF),
                   jax.ShapeDtypeStruct((ROOM,), jnp.int32)),
        in_specs=[hbm] * len(args),
        out_specs=(hbm, hbm, hbm, hbm),
        scratch_shapes=[
            pltpu.SMEM((batch,), jnp.int32),
            pltpu.VMEM(table.shape, F32),
            pltpu.VMEM((batch, table.shape[1]), F32),
            rows, rows, rows,
            pltpu.VMEM((BLK * 8, 128), F32),
            pltpu.VMEM((2, BLK // 2, 16, 256), F32),
            pltpu.VMEM((batch, qcols), BF),
            pltpu.VMEM((nblk, BLK) + k_cache.shape[2:], BF),
            pltpu.VMEM((nblk, BLK) + v_cache.shape[2:], BF),
            pltpu.VMEM(hidden.shape, BF), pltpu.VMEM(norm.shape, BF), pltpu.VMEM((dim, cols), BF), pltpu.VMEM(hidden.shape, BF),
            pltpu.SemaphoreType.DMA((9,)),
            pltpu.SemaphoreType.DMA((2, nblk)),
            pltpu.SemaphoreType.DMA((2, nblk)),
        ],
        compiler_params=pltpu.CompilerParams(vmem_limit_bytes=62 * 2**20),
        cost_estimate=pl.CostEstimate(flops=2 * batch * dim * cols, bytes_accessed=76 * 2**20, transcendentals=0),
        name=f"attn{layer}",
    )(*args)


COPY_HOLD = 11


def write_kernel(layer, pos_hbm, new_hbm, k_hbm, v_hbm, k_prev, v_prev, ko_hbm, vo_hbm, pos_ref, new, k_rows, v_rows, kbuf, vbuf, sem, insem, outsem):
    nblk = kbuf.shape[0]
    batch = nblk * BLK
    first = [pltpu.make_async_copy(pos_hbm.at[pl.ds(0, batch)], pos_ref, sem.at[0]), pltpu.make_async_copy(new_hbm.at[0], new, sem.at[1])]
    for c in first:
        c.start()

    def in_copies(i):
        rows = pl.ds(i * BLK, BLK)
        return (pltpu.make_async_copy(k_hbm.at[layer, rows], kbuf.at[i], insem.at[0, i]),
                pltpu.make_async_copy(v_hbm.at[layer, rows], vbuf.at[i], insem.at[1, i]))

    def out_copies(i):
        rows = pl.ds(i * BLK, BLK)
        return (pltpu.make_async_copy(kbuf.at[i], ko_hbm.at[layer, rows], outsem.at[0, i]),
                pltpu.make_async_copy(vbuf.at[i], vo_hbm.at[layer, rows], outsem.at[1, i]))

    @pl.loop(0, nblk)
    def _(i):
        for c in in_copies(i):
            c.start()

    for c in first:
        c.wait()
    for h in range(2):
        k_vec = new[h].astype(F32)
        v_vec = new[2 + h].astype(F32)
        for r in range(4):
            k_rows[pl.ds(2 * r + h, batch, stride=8), :] = k_vec
            v_rows[pl.ds(2 * r + h, batch, stride=8), :] = v_vec

    @pl.loop(0, nblk)
    def _(i):
        for c in in_copies(i):
            c.wait()
        patch(kbuf, vbuf, k_rows, v_rows, pos_ref, i)

        @pl.when(i == COPY_HOLD)
        def _():
            @pl.loop(0, COPY_HOLD)
            def _(j):
                for c in out_copies(j):
                    c.start()

        @pl.when(i >= COPY_HOLD)
        def _():
            for c in out_copies(i):
                c.start()

    @pl.loop(0, nblk)
    def _(i):
        for c in out_copies(i):
            c.wait()


def write_rows(layer, positions, new, k_cache, v_cache, prev):
    batch = k_cache.shape[1]
    nblk = batch // BLK
    anyspec = pl.BlockSpec(memory_space=pltpu.HBM)
    return pl.pallas_call(
        functools.partial(write_kernel, layer),
        out_shape=(jax.ShapeDtypeStruct(k_cache.shape, BF), jax.ShapeDtypeStruct(v_cache.shape, BF)),
        in_specs=[anyspec] * 6,
        out_specs=(anyspec, anyspec),
        scratch_shapes=[
            pltpu.SMEM((batch,), jnp.int32),
            pltpu.VMEM(new.shape[1:], BF),
            pltpu.VMEM((batch * 8, 128), F32),
            pltpu.VMEM((batch * 8, 128), F32),
            pltpu.VMEM((nblk, BLK) + k_cache.shape[2:], BF),
            pltpu.VMEM((nblk, BLK) + v_cache.shape[2:], BF),
            pltpu.SemaphoreType.DMA((2,)),
            pltpu.SemaphoreType.DMA((2, nblk)),
            pltpu.SemaphoreType.DMA((2, nblk)),
        ],
        input_output_aliases={4: 0, 5: 1},
        compiler_params=pltpu.CompilerParams(vmem_limit_bytes=50 * 2**20),
        cost_estimate=pl.CostEstimate(flops=0, bytes_accessed=67 * 2**20, transcendentals=0),
        name="write_rows",
    )(positions, new, k_cache, v_cache, *prev)


CW = 512
HALF = 128
GC = 8
SPARE = 64
SLOT = 8


def mega_kernel(pos_hbm, table_hbm, att_hbm, x_hbm, mnorm_hbm, anorm_hbm, wo_hbm, wg_hbm, wu_hbm, wd_hbm, wq_hbm, wk_hbm, wv_hbm, k_hbm, v_hbm,
                out_hbm, new_hbm,
                pos_ref, table, cs, wo, wg, wu, wd, wqkv, att, x, mnorm, anorm, h, act, qkv, q_rows, k_rows, v_rows, o_rows, s_buf, new,
                own, sd, sx, rd, rx,
                wosem, gsem, usem, wsem, isem, hsem, sd_sem, sx_sem, sg_sem, rd_sem, rx_sem, ra_sem, osem):
    dim = x.shape[1]
    nch = dim // 2 // CW
    ncol = wg.shape[0]
    qcols = wq_hbm.shape[2]
    kcols = wk_hbm.shape[2]
    heads = qcols // 128
    tp = lax.axis_index("tp")
    core = lax.rem(tp, 2)
    sib = tp + 1 - 2 * core
    peer = lax.rem(tp + 2, 4)
    mine = pl.multiple_of(core * (dim // 2), CW)
    theirs = pl.multiple_of((1 - core) * (dim // 2), CW)

    def chunk(side, k):
        return pl.ds(pl.multiple_of((theirs, mine)[side] + k * CW, CW), CW)

    def wo_copy(layer, side, k):
        return pltpu.make_async_copy(wo_hbm.at[layer, :, chunk(side, k)], wo.at[:, chunk(side, k)], wosem.at[side, k])

    def gu_copies(layer, c):
        cols = pl.ds(pl.multiple_of(c * 128, 128), 128)
        return (pltpu.make_async_copy(wg_hbm.at[layer, :, cols], wg.at[c], gsem.at[c]),
                pltpu.make_async_copy(wu_hbm.at[layer, :, cols], wu.at[c], usem.at[c]))

    def kv_copies(half, c):
        src = pl.ds(pl.multiple_of((half * HALF + c * SLOT) * 256, 2048), SLOT * 256)
        dst = pl.ds(0, SLOT * 256)
        return (pltpu.make_async_copy(k_hbm.at[1, src], wg.at[c, dst], gsem.at[c]),
                pltpu.make_async_copy(v_hbm.at[1, src], wu.at[c, dst], usem.at[c]))

    def wd_copy(layer):
        return pltpu.make_async_copy(wd_hbm.at[layer], wd, wsem.at[0])

    def half_copy(which, half):
        rows = pl.ds(half * HALF, HALF)
        src, dst = ((att_hbm, att), (x_hbm, x))[which]
        return pltpu.make_async_copy(src.at[rows], dst.at[rows], hsem.at[which, half])

    small = [pltpu.make_async_copy(mnorm_hbm, mnorm, isem.at[2]), pltpu.make_async_copy(anorm_hbm, anorm, isem.at[3]),
             pltpu.make_async_copy(pos_hbm, pos_ref, isem.at[4]), pltpu.make_async_copy(table_hbm, table, isem.at[5])]
    qkv_loads = [
        pltpu.make_async_copy(wq_hbm.at[1], wqkv.at[:, pl.ds(0, qcols)], wsem.at[1]),
        pltpu.make_async_copy(wk_hbm.at[1], wqkv.at[:, pl.ds(qcols, kcols)], wsem.at[2]),
        pltpu.make_async_copy(wv_hbm.at[1], wqkv.at[:, pl.ds(qcols + kcols, kcols)], wsem.at[3]),
    ]
    half_copy(0, 0).start()
    wo_copy(0, 0, 0).start()
    half_copy(1, 0).start()
    wo_copy(0, 0, 1).start()
    wo_copy(0, 1, 0).start()
    for k in range(2, nch):
        wo_copy(0, 0, k).start()
    for k in range(1, nch):
        wo_copy(0, 1, k).start()
    half_copy(0, 1).start()
    half_copy(1, 1).start()
    for c in small:
        c.start()

    barrier = pltpu.get_barrier_semaphore()
    for other in (sib, peer):
        pl.semaphore_signal(barrier, inc=1, device_id={"tp": other}, device_id_type=MESH)
    pl.semaphore_wait(barrier, 2)

    def to_sib(ph, k):
        return pltpu.make_async_remote_copy(sd.at[ph % 2, k], rd.at[ph % 4, k], sd_sem.at[ph, k], rd_sem.at[ph, k],
                                            device_id={"tp": sib}, device_id_type=MESH)

    def to_peer(ph, k):
        return pltpu.make_async_remote_copy(sx.at[ph % 2, k], rx.at[ph % 4, k], sx_sem.at[ph, k], rx_sem.at[ph, k],
                                            device_id={"tp": peer}, device_id_type=MESH)

    def final(ph):
        return ph >= 6

    def share(ph, k):
        rows = pl.ds((ph % 2) * HALF, HALF)
        dst = out_hbm if final(ph) else x
        return pltpu.make_async_remote_copy(x.at[rows, chunk(1, k)], dst.at[rows, chunk(1, k)], sg_sem.at[ph, k], ra_sem.at[ph, k],
                                            device_id={"tp": sib}, device_id_type=MESH)

    def keep(ph, k):
        rows = pl.ds((ph % 2) * HALF, HALF)
        return pltpu.make_async_copy(x.at[rows, chunk(1, k)], out_hbm.at[rows, chunk(1, k)], osem.at[ph % 2, k])

    def reduce_start(ph, lhs, w_ref, load):
        def dot(side, k):
            if load is not None:
                load(side, k).wait()
            return jnp.dot(lhs(), w_ref[:, chunk(side, k)], preferred_element_type=F32)

        def send(k):
            sd[ph % 2, k] = dot(0, k).astype(BF)
            to_sib(ph, k).start()

        def hold(k):
            own[k] = dot(1, k)

        def forward(k):
            to_sib(ph, k).wait_recv()
            sx[ph % 2, k] = (own[k] + rd[ph % 4, k].astype(F32)).astype(BF)
            to_peer(ph, k).start()

        send(0)
        send(1)
        hold(0)
        for k in range(2, nch):
            send(k)
        forward(0)

        def rest():
            for k in range(1, nch):
                hold(k)
                forward(k)
            for k in range(nch):
                to_sib(ph, k).wait_send()

        return rest

    def reduce_end(ph, between=None):
        rows = pl.ds((ph % 2) * HALF, HALF)
        for k in range(nch):
            to_peer(ph, k).wait()
            total = (sx[ph % 2, k].astype(F32) + rx[ph % 4, k].astype(F32)).astype(BF)
            x[rows, chunk(1, k)] = (x[rows, chunk(1, k)].astype(F32) + total.astype(F32)).astype(BF)
            share(ph, k).start()
            if final(ph):
                keep(ph, k).start()
        if between is not None:
            between()
        for k in range(nch):
            share(ph, k).wait()

    def gate_up(layer, half):
        rows = pl.ds(half * HALF, HALF)
        h[...] = normed(x[rows, :].astype(F32), mnorm[layer:layer + 1, :].astype(F32))

        @pl.loop(0, ncol // GC)
        def _(n):
            if half == 0:
                for c in range(GC):
                    for cp in gu_copies(layer, n * GC + c):
                        cp.wait()
            wide = lambda ref: jnp.concatenate([ref[n * GC + c] for c in range(GC)], axis=1)
            g = jnp.dot(h[...], wide(wg), preferred_element_type=F32).astype(BF).astype(F32)
            u = jnp.dot(h[...], wide(wu), preferred_element_type=F32).astype(BF).astype(F32)
            cols = pl.ds(pl.multiple_of(n * GC * 128, GC * 128), GC * 128)
            act[:, cols] = (g * jax.nn.sigmoid(g) * u).astype(BF)

    def qkv_rope(half):
        rows = pl.ds(half * HALF, HALF)
        h[...] = normed(x[rows, :].astype(F32), anorm[1:2, :].astype(F32))

        full = jnp.dot(h[...], wqkv[...], preferred_element_type=F32).astype(BF)
        for n in range(qkv.shape[0]):
            qkv[n] = full[:, n * 256:(n + 1) * 256]

        cos_b = cs[rows, 0:128]
        sin_b = cs[rows, 128:256]

        def piece(n, i):
            return qkv[n, :, i * 128:i * 128 + 128].astype(F32)

        def rope(vec):
            return (vec * cos_b + pltpu.roll(vec, 64, 1) * sin_b).astype(BF)

        k_new = [rope(piece(heads // 2, i)) for i in range(2)]
        v_new = [piece(heads // 2 + 1, i) for i in range(2)]
        for i in range(2):
            new[i, rows, :] = k_new[i]
            new[2 + i, rows, :] = v_new[i].astype(BF)
        zero = jnp.zeros((HALF, 128), F32)
        for j in range(8):
            out_rows = pl.ds(j, HALF, stride=8)
            kv = 0 if j < heads // 2 else 1
            q_rows[out_rows, :] = rope(piece(j // 2, j % 2)).astype(F32) if j < heads else zero
            k_rows[out_rows, :] = k_new[kv].astype(F32)
            v_rows[out_rows, :] = v_new[kv]

    col = lax.broadcasted_iota(jnp.int32, (8, 256), 1)
    row = lax.broadcasted_iota(jnp.int32, (8, 256), 0)
    key_row = jnp.where((col & 1) == jnp.where(row >= heads // 2, 1, 0), col >> 1, 4096)
    scale = 128 ** -0.5

    def attend(half):
        pairs = range(SLOT)
        zero8 = jnp.zeros((8, 128), F32)
        steps = ncol // 2

        def rows8(i, p, b):
            return pl.ds(pl.multiple_of((i * 2 * SLOT + 2 * p + b) * 8, 8), 8)

        def both(ref, i, p):
            r = 2 * p % SLOT
            slot = 2 * i + 2 * p // SLOT
            return jnp.concatenate([ref[slot, r * 256:(r + 1) * 256, :], ref[slot, (r + 1) * 256:(r + 2) * 256, :]], axis=1)

        def score(i):
            for p in pairs:
                qa = q_rows[rows8(i, p, 0), :]
                qb = q_rows[rows8(i, p, 1), :]
                q2 = jnp.concatenate([jnp.concatenate([qa, zero8], axis=1), jnp.concatenate([zero8, qb], axis=1)], axis=0).astype(BF)
                s_buf[lax.rem(i, 2), p] = lax.dot_general(q2, both(wg, i, p), (((1,), (1,)), ((), ())), preferred_element_type=F32)

        def step(i, more):
            if more:
                for c in range(2):
                    kv_copies(half, 2 * i + 2 + c)[0].wait()
            for c in range(2):
                kv_copies(half, 2 * i + c)[1].wait()
            scores = [s_buf[lax.rem(i, 2), p] for p in pairs]
            if more:
                score(i + 1)
            weights, last = [], []
            for p in pairs:
                prod = jnp.concatenate([q_rows[rows8(i, p, b), :] * k_rows[rows8(i, p, b), :] for b in range(2)], axis=0)
                fresh = jnp.sum(prod, axis=-1, keepdims=True) * scale
                pos = [pos_ref[half * HALF + i * 2 * SLOT + 2 * p + b] for b in range(2)]
                before = jnp.concatenate([key_row < pos[0], key_row < pos[1]], axis=0)
                s = jnp.where(before, scores[p] * scale, NEG)
                peak = jnp.maximum(jnp.max(s, axis=-1, keepdims=True), fresh)
                e = jnp.exp(s - peak)
                e_new = jnp.exp(fresh - peak)
                inv = 1.0 / (jnp.sum(e, axis=-1, keepdims=True) + e_new)
                weights.append((e * inv).astype(BF))
                last.append((e_new * inv).astype(BF).astype(F32))
            outs = [jnp.dot(weights[p], both(wu, i, p), preferred_element_type=F32) for p in pairs]
            for p in pairs:
                o_rows[rows8(i, p, 0), :] = outs[p][0:8, 0:128] + last[p][0:8] * v_rows[rows8(i, p, 0), :]
                o_rows[rows8(i, p, 1), :] = outs[p][8:16, 128:256] + last[p][8:16] * v_rows[rows8(i, p, 1), :]
            for c in range(2):
                for cp in (kv_copies(1, 2 * i + c) if half == 0 else gu_copies(1, 2 * i + c)):
                    cp.start()

        for c in range(2):
            kv_copies(half, c)[0].wait()
        score(0)

        @pl.loop(0, steps - 1)
        def _(i):
            step(i, True)

        step(steps - 1, False)

        rows = pl.ds(half * HALF, HALF)
        for j in range(heads):
            att[rows, j * 128:(j + 1) * 128] = o_rows[pl.ds(j, HALF, stride=8), :].astype(BF)

    def att_half(half):
        return lambda: att[half * HALF:(half + 1) * HALF, :]

    half_copy(0, 0).wait()
    half_copy(1, 0).wait()
    reduce_start(0, att_half(0), wo, lambda side, k: wo_copy(0, side, k))()

    @pl.loop(0, ncol)
    def _(c):
        for cp in gu_copies(0, c):
            cp.start()

    wd_copy(0).start()
    for c in qkv_loads:
        c.start()
    half_copy(0, 1).wait()
    half_copy(1, 1).wait()
    rest = reduce_start(1, att_half(1), wo, None)
    for c in small:
        c.wait()

    @pl.loop(0, 2 * HALF // 8)
    def _(i):
        for b in range(8):
            r = i * 8 + b
            cs[pl.ds(r, 1), :] = table[pl.ds(pos_ref[r], 1), :]

    for half in range(2):
        reduce_end(half, rest)
        if half == 0:
            for k in range(nch):
                wo_copy(1, 0, k).start()
                wo_copy(1, 1, k).start()
        gate_up(0, half)
        if half == 0:
            wd_copy(0).wait()
        else:
            @pl.loop(0, ncol)
            def _(c):
                for cp in kv_copies(0, c):
                    cp.start()

        rest = reduce_start(2 + half, lambda: act[...], wd, None)
    for half in range(2):
        reduce_end(2 + half, rest)
        if half == 0:
            wd_copy(1).start()
            for c in qkv_loads:
                c.wait()
        qkv_rope(half)
        attend(half)
        rest = reduce_start(4 + half, att_half(half), wo, (lambda side, k: wo_copy(1, side, k)) if half == 0 else None)
    new_copy = pltpu.make_async_copy(new, new_hbm.at[0], isem.at[6])
    new_copy.start()
    for half in range(2):
        reduce_end(4 + half, rest)
        gate_up(1, half)
        if half == 0:
            wd_copy(1).wait()
        rest = reduce_start(6 + half, lambda: act[...], wd, None)
    reduce_end(6, rest)
    reduce_end(7)
    new_copy.wait()
    for half in range(2):
        for k in range(nch):
            keep(6 + half, k).wait()


def mega(positions, table, att, hidden, mnorm, anorm, wo, wg, wu, wd, wq, wk, wv, k_rows, v_rows):
    batch, dim = hidden.shape
    nch = dim // 2 // CW
    cols = wq.shape[2] + 2 * wk.shape[2]
    ncol = wg.shape[2] // 128
    anyspec = pl.BlockSpec(memory_space=pl.ANY)
    msg = lambda n: pltpu.VMEM((n, nch, HALF, CW), BF)
    sems = pltpu.SemaphoreType.DMA((8, nch))
    rows = pltpu.VMEM((HALF * 8, 128), F32)
    args = [positions, table, att, hidden, mnorm, anorm, wo, wg, wu, wd, wq, wk, wv, k_rows, v_rows]
    return pl.pallas_call(
        mega_kernel,
        out_shape=(jax.ShapeDtypeStruct((batch, dim), BF), jax.ShapeDtypeStruct((SPARE, 4, batch, 128), BF)),
        in_specs=[anyspec] * len(args),
        out_specs=(anyspec, anyspec),
        scratch_shapes=[
            pltpu.SMEM((batch,), jnp.int32), pltpu.VMEM(table.shape, F32), pltpu.VMEM((batch, table.shape[1]), F32),
            pltpu.VMEM(wo.shape[1:], BF), pltpu.VMEM((ncol, dim, 128), BF), pltpu.VMEM((ncol, dim, 128), BF), pltpu.VMEM(wd.shape[1:], BF),
            pltpu.VMEM((dim, cols), BF), pltpu.VMEM(att.shape, BF), pltpu.VMEM(hidden.shape, BF),
            pltpu.VMEM(mnorm.shape, BF), pltpu.VMEM(anorm.shape, BF),
            pltpu.VMEM((HALF, dim), BF), pltpu.VMEM((HALF, wd.shape[1]), BF), pltpu.VMEM((cols // 256, HALF, 256), BF),
            rows, rows, rows, rows, pltpu.VMEM((2, SLOT, 16, 256), F32), pltpu.VMEM((4, batch, 128), BF),
            pltpu.VMEM((nch, HALF, CW), F32), msg(2), msg(2), msg(4), msg(4),
            pltpu.SemaphoreType.DMA((2, nch)), pltpu.SemaphoreType.DMA((ncol,)), pltpu.SemaphoreType.DMA((ncol,)),
            pltpu.SemaphoreType.DMA((4,)), pltpu.SemaphoreType.DMA((7,)), pltpu.SemaphoreType.DMA((2, 2)),
            sems, sems, sems, sems, sems, sems, pltpu.SemaphoreType.DMA((2, nch)),
        ],
        compiler_params=pltpu.CompilerParams(collective_id=0, has_side_effects=True, vmem_limit_bytes=67043328),
        name="mega",
    )(*args)


def solution(mesh):
    row_spec = P('dp', None)
    pos_spec = P('dp')
    cache_spec = P(None, 'dp', None, 'tp', None)
    norm_spec = P(None, None)
    col_spec = P(None, None, 'tp')
    split_rows = P(None, 'tp', None)

    def local_step(hidden, positions, k_cache, v_cache, attn_norm, w_query, w_key, w_value, w_out, mlp_norm, w_gate, w_up, w_down):
        cache_shape = k_cache.shape
        flat = (cache_shape[0], cache_shape[1], cache_shape[2] * cache_shape[3], cache_shape[4])
        k_flat, v_flat = k_cache.reshape(flat), v_cache.reshape(flat)
        table = jnp.asarray(rope_table(cache_shape[2], cache_shape[4]))
        att, *caches, where = attention(0, positions, table, hidden, attn_norm, w_query, w_key, w_value, k_flat, v_flat)
        rows = (cache_shape[0], -1, cache_shape[4])
        hidden, new = mega(positions, table, att, hidden, mlp_norm, attn_norm, w_out, w_gate, w_up, w_down, w_query, w_key, w_value,
                           k_cache.reshape(rows), v_cache.reshape(rows))
        caches = write_rows(1, where, new, k_flat, v_flat, caches)
        return hidden, caches[0].reshape(cache_shape), caches[1].reshape(cache_shape)

    return jax.shard_map(local_step, mesh=mesh, in_specs=(row_spec, pos_spec, cache_spec, cache_spec, norm_spec, col_spec, col_spec, col_spec, split_rows, norm_spec, col_spec, col_spec, split_rows), out_specs=(row_spec, cache_spec, cache_spec), check_vma=False)
```
